32 devices in a mesh: data: 1 (over z), pp: 4 (over y), ep: 8 (over x, core).
Axes of the slice: x: 4, y: 4, z: 1, core: 2. Of those that a mesh axis runs over, the one named last changes fastest.
The devices are a block of a 4x4x8 slice.
Arguments:
- expert_out: bfloat16 [4, 2, 256, 128, 2048], P('pp', 'data', 'ep')
- expert_ids: int32 [4, 2, 32, 64, 8], P('pp', 'data', 'ep')
- slot_ids: int32 [4, 2, 32, 64, 8], P('pp', 'data', 'ep')
- gate_weights: float32 [4, 2, 32, 64, 8], P('pp', 'data', 'ep')
- residual: bfloat16 [4, 2, 32, 64, 2048], P('pp', 'data', 'ep')
- norm_moe: float32 [4, 2048], P('pp')
- w_gate: bfloat16 [4, 2048, 512], P('pp')
- w_up: bfloat16 [4, 2048, 512], P('pp')
- w_down: bfloat16 [4, 512, 2048], P('pp')
- norm_attn: float32 [4, 2048], P('pp')
- w_query: bfloat16 [4, 2048, 16, 128], P('pp')
- w_key: bfloat16 [4, 2048, 16, 128], P('pp')
- w_value: bfloat16 [4, 2048, 16, 128], P('pp')
- w_out: bfloat16 [4, 16, 128, 2048], P('pp')
Outputs:
- output: bfloat16 [4, 2, 32, 64, 2048], P('pp', 'data', 'ep')
All inputs are finite; a program needn't handle non-finite values.
Results may differ from the reference program's by a relative error of at most 0.0154484.
Values are sent between devices in bfloat16 or wider.
A program may use at most 768 MiB of HBM per device.

```python
import math
import jax
import jax.numpy as jnp
from jax import lax

STAGES = 4
EP_SIZE = 8
MICRO_BATCHES = 2
SEQ_DEV = 4
SEQ_LEN = 64
D_MODEL = 2048
NUM_HEADS = 16
HEAD_DIM = 128
EXPERTS = 256
TOP_K = 8
FF_SHARED = 512
CAP_SLOTS = 16

SEQS = EP_SIZE * SEQ_DEV
TOK_DEV = SEQ_DEV * SEQ_LEN
TOKENS = SEQS * SEQ_LEN
SLOTS = EP_SIZE * CAP_SLOTS
HEADS_WIDTH = NUM_HEADS * HEAD_DIM
SCORE_SCALE = 1.0 / math.sqrt(HEAD_DIM)
EPSILON = 1e-6


def route_group(group_args):
    group_key, hot_draw = group_args
    hot_rank = jnp.argsort(jnp.argsort(hot_draw * EXPERTS + jnp.arange(EXPERTS)))
    lead_mask = (jnp.arange(TOK_DEV) <= CAP_SLOTS).astype(jnp.int32)[:, None]
    hot_bias = jnp.where(hot_rank < max(1, TOP_K // 4), 1024, 0) + jnp.where(hot_rank == 0, 8192, 0) * lead_mask
    noise_draw = jax.random.randint(group_key, (EP_SIZE, TOK_DEV, EXPERTS), 0, 4096)
    scores = (noise_draw + hot_bias) * EXPERTS + jnp.arange(EXPERTS)
    top_vals, expert_ids = lax.top_k(scores, TOP_K)
    choice_count = TOK_DEV * TOP_K
    flat_ids = expert_ids.reshape(EP_SIZE, choice_count)
    position = jnp.arange(choice_count)
    sort_order = jnp.argsort(flat_ids * choice_count + position, axis=-1)
    sorted_ids = jnp.take_along_axis(flat_ids, sort_order, axis=-1)
    is_start = jnp.concatenate([jnp.ones((EP_SIZE, 1), jnp.bool_), sorted_ids[:, 1:] != sorted_ids[:, :-1]], axis=1)
    start_pos = lax.cummax(jnp.where(is_start, position, 0), axis=1)
    slot_rank = jnp.take_along_axis(position - start_pos, jnp.argsort(sort_order, axis=-1), axis=-1)
    source = jnp.arange(EP_SIZE)[:, None]
    slot_ids = jnp.where(slot_rank < CAP_SLOTS, source * CAP_SLOTS + slot_rank, -1)
    return expert_ids.reshape(SEQS, SEQ_LEN, TOP_K), slot_ids.reshape(SEQS, SEQ_LEN, TOP_K)


def draw_routing(key):
    key_hot, key_score = jax.random.split(key)
    hot_draw = jax.random.randint(key_hot, (STAGES * MICRO_BATCHES, EXPERTS), 0, 1 << 20)
    group_keys = jax.random.split(key_score, STAGES * MICRO_BATCHES)
    expert_ids, slot_ids = lax.map(route_group, (group_keys, hot_draw))
    route_shape = (STAGES, MICRO_BATCHES, SEQS, SEQ_LEN, TOP_K)
    return expert_ids.reshape(route_shape), slot_ids.reshape(route_shape)


def setup_inputs(seed: int = 0, part: int = 0) -> dict:
    base_key = jax.random.key(seed)
    part_keys = jax.random.split(jax.random.fold_in(base_key, part), 5)
    expert_ids, slot_ids = draw_routing(part_keys[0])
    route_shape = (STAGES, MICRO_BATCHES, SEQS, SEQ_LEN, TOP_K)
    gate_draw = jax.random.normal(part_keys[1], route_shape, jnp.float32)
    gate_weights = jnp.exp(1.2 * gate_draw - 0.72) / TOP_K
    expert_scale = jax.random.uniform(part_keys[2], (STAGES * MICRO_BATCHES, EXPERTS, 1, 1), jnp.float32, 0.5, 3.0)
    out_keys = jax.random.split(part_keys[3], STAGES * MICRO_BATCHES)

    def draw_outputs(group_args):
        group_key, group_scale = group_args
        normal_draw = jax.random.normal(group_key, (EXPERTS, SLOTS, D_MODEL), jnp.float32)
        return (normal_draw * group_scale).astype(jnp.bfloat16)

    expert_out = lax.map(draw_outputs, (out_keys, expert_scale)).reshape(STAGES, MICRO_BATCHES, EXPERTS, SLOTS, D_MODEL)
    residual = jax.random.normal(part_keys[4], (STAGES, MICRO_BATCHES, SEQS, SEQ_LEN, D_MODEL), jnp.float32).astype(jnp.bfloat16)
    weight_keys = jax.random.split(jax.random.key(seed + 1), 9)
    in_scale = 1.0 / math.sqrt(D_MODEL)
    down_scale = 2.0 / math.sqrt(FF_SHARED)
    query_scale = 1.5 / math.sqrt(D_MODEL)
    out_scale = math.sqrt(math.sqrt(SEQ_LEN)) / math.sqrt(HEADS_WIDTH)
    norm_moe = jax.random.uniform(weight_keys[0], (STAGES, D_MODEL), jnp.float32, 0.5, 1.5)
    w_gate = (jax.random.normal(weight_keys[1], (STAGES, D_MODEL, FF_SHARED), jnp.float32) * in_scale).astype(jnp.bfloat16)
    w_up = (jax.random.normal(weight_keys[2], (STAGES, D_MODEL, FF_SHARED), jnp.float32) * in_scale).astype(jnp.bfloat16)
    w_down = (jax.random.normal(weight_keys[3], (STAGES, FF_SHARED, D_MODEL), jnp.float32) * down_scale).astype(jnp.bfloat16)
    norm_attn = jax.random.uniform(weight_keys[4], (STAGES, D_MODEL), jnp.float32, 0.5, 1.5)
    w_query = (jax.random.normal(weight_keys[5], (STAGES, D_MODEL, NUM_HEADS, HEAD_DIM), jnp.float32) * query_scale).astype(jnp.bfloat16)
    w_key = (jax.random.normal(weight_keys[6], (STAGES, D_MODEL, NUM_HEADS, HEAD_DIM), jnp.float32) * in_scale).astype(jnp.bfloat16)
    w_value = (jax.random.normal(weight_keys[7], (STAGES, D_MODEL, NUM_HEADS, HEAD_DIM), jnp.float32) * in_scale).astype(jnp.bfloat16)
    w_out = (jax.random.normal(weight_keys[8], (STAGES, NUM_HEADS, HEAD_DIM, D_MODEL), jnp.float32) * out_scale).astype(jnp.bfloat16)
    return {"expert_out": expert_out, "expert_ids": expert_ids, "slot_ids": slot_ids, "gate_weights": gate_weights, "residual": residual, "norm_moe": norm_moe, "w_gate": w_gate, "w_up": w_up, "w_down": w_down, "norm_attn": norm_attn, "w_query": w_query, "w_key": w_key, "w_value": w_value, "w_out": w_out}


def rms_norm(tensor, gain):
    values = tensor.astype(jnp.float32)
    inv_rms = lax.rsqrt(jnp.mean(values * values, axis=-1, keepdims=True) + EPSILON)
    return values * inv_rms * gain


def shared_expert(residual, norm_moe, w_gate, w_up, w_down):
    normed = rms_norm(residual, norm_moe).astype(jnp.bfloat16)
    gate_act = jnp.dot(normed, w_gate, preferred_element_type=jnp.float32)
    up_act = jnp.dot(normed, w_up, preferred_element_type=jnp.float32)
    hidden = (jax.nn.silu(gate_act) * up_act).astype(jnp.bfloat16)
    return jnp.dot(hidden, w_down, preferred_element_type=jnp.float32).astype(jnp.bfloat16)


def combine_micro(micro_args, stage_weights):
    expert_out, expert_ids, slot_ids, gate_weights, residual = micro_args
    norm_moe, w_gate, w_up, w_down = stage_weights
    flat_slots = slot_ids.reshape(TOKENS, TOP_K)
    kept_mask = flat_slots >= 0
    row_ids = expert_ids.reshape(TOKENS, TOP_K) * SLOTS + jnp.where(kept_mask, flat_slots, 0)
    picked = jnp.take(expert_out.reshape(EXPERTS * SLOTS, D_MODEL), row_ids, axis=0)
    weights = jnp.where(kept_mask, gate_weights.reshape(TOKENS, TOP_K), 0.0)
    routed = jnp.sum(picked.astype(jnp.float32) * weights[:, :, None], axis=1)
    flat_resid = residual.reshape(TOKENS, D_MODEL)
    shared = shared_expert(flat_resid, norm_moe, w_gate, w_up, w_down)
    combined = flat_resid.astype(jnp.float32) + shared.astype(jnp.float32) + routed
    return combined.astype(jnp.bfloat16).reshape(SEQS, SEQ_LEN, D_MODEL)


def attend_sequence(seq_args):
    queries, key_heads, value_heads = seq_args
    scores = jnp.einsum("qhe,khe->hqk", queries.astype(jnp.float32), key_heads.astype(jnp.float32)) * SCORE_SCALE
    causal = jnp.arange(SEQ_LEN)[:, None] >= jnp.arange(SEQ_LEN)[None, :]
    scores = jnp.where(causal, scores, -1e30)
    attn_probs = jnp.exp(scores - jnp.max(scores, axis=-1, keepdims=True))
    prob_sum = jnp.sum(attn_probs, axis=-1, keepdims=True)
    attn_mixed = jnp.einsum("hqk,khe->hqe", attn_probs.astype(jnp.bfloat16).astype(jnp.float32), value_heads.astype(jnp.float32))
    return attn_mixed / prob_sum


def attention_stage(stage_args):
    received, norm_attn, w_query, w_key, w_value, w_out = stage_args
    seq_count = MICRO_BATCHES * SEQS
    normed = rms_norm(received, norm_attn).astype(jnp.bfloat16).reshape(seq_count * SEQ_LEN, D_MODEL)

    def project(weight):
        product = jnp.dot(normed, weight.reshape(D_MODEL, HEADS_WIDTH), preferred_element_type=jnp.float32)
        return product.astype(jnp.bfloat16).reshape(seq_count, SEQ_LEN, NUM_HEADS, HEAD_DIM)

    attn_mixed = lax.map(attend_sequence, (project(w_query), project(w_key), project(w_value)))
    mixed_rows = jnp.transpose(attn_mixed.astype(jnp.bfloat16), (0, 2, 1, 3)).reshape(seq_count * SEQ_LEN, HEADS_WIDTH)
    attn_proj = jnp.dot(mixed_rows, w_out.reshape(HEADS_WIDTH, D_MODEL), preferred_element_type=jnp.float32).astype(jnp.bfloat16)
    updated = received.astype(jnp.float32) + attn_proj.astype(jnp.float32).reshape(received.shape)
    return updated.astype(jnp.bfloat16)


def reference(expert_out, expert_ids, slot_ids, gate_weights, residual, norm_moe, w_gate, w_up, w_down, norm_attn, w_query, w_key, w_value, w_out):
    def combine_stage(stage_args):
        def one_micro(micro_args):
            return combine_micro(micro_args, stage_args[5:])
        return lax.map(one_micro, stage_args[:5])

    combined = lax.map(combine_stage, (expert_out, expert_ids, slot_ids, gate_weights, residual, norm_moe, w_gate, w_up, w_down))
    received = jnp.roll(combined, 1, axis=0)
    return lax.map(attention_stage, (received, norm_attn, w_query, w_key, w_value, w_out))
```

```python
import functools
import math
import jax
import jax.numpy as jnp
from jax import lax
from jax.experimental import pallas as pl
from jax.experimental.pallas import tpu as pltpu
from jax.sharding import PartitionSpec as P

EPSILON = 1e-6
CORES = 2
MESH = pl.DeviceIdType.MESH
BF16_MAX = 3.3895313892515355e38


def rms_norm(tensor, gain):
    values = tensor.astype(jnp.float32)
    inv_rms = lax.rsqrt(jnp.mean(values * values, axis=-1, keepdims=True) + EPSILON)
    return values * inv_rms * gain


def shared_expert(residual, norm_moe, w_gate, w_up, w_down):
    normed = rms_norm(residual, norm_moe).astype(jnp.bfloat16)
    gate_act = jnp.einsum("bld,df->blf", normed, w_gate, preferred_element_type=jnp.float32)
    up_act = jnp.einsum("bld,df->blf", normed, w_up, preferred_element_type=jnp.float32)
    hidden = (jax.nn.silu(gate_act) * up_act).astype(jnp.bfloat16)
    return jnp.einsum("blf,fd->bld", hidden, w_down, preferred_element_type=jnp.float32).astype(jnp.bfloat16)


def attention_block(combined, norm_attn, w_query, w_key, w_value, w_out):
    seq_len = combined.shape[1]
    score_scale = 1.0 / math.sqrt(w_query.shape[2])
    normed = rms_norm(combined, norm_attn).astype(jnp.bfloat16)
    queries = jnp.einsum("bld,dhe->blhe", normed, w_query, preferred_element_type=jnp.float32).astype(jnp.bfloat16)
    key_heads = jnp.einsum("bld,dhe->blhe", normed, w_key, preferred_element_type=jnp.float32).astype(jnp.bfloat16)
    value_heads = jnp.einsum("bld,dhe->blhe", normed, w_value, preferred_element_type=jnp.float32).astype(jnp.bfloat16)
    scores = jnp.einsum("bqhe,bkhe->bhqk", queries, key_heads, preferred_element_type=jnp.float32) * score_scale
    causal = jnp.arange(seq_len)[:, None] >= jnp.arange(seq_len)[None, :]
    scores = jnp.where(causal, scores, -1e30)
    attn_probs = jnp.exp(scores - jnp.max(scores, axis=-1, keepdims=True))
    prob_sum = jnp.sum(attn_probs, axis=-1, keepdims=True)
    attn_mixed = jnp.einsum("bhqk,bkhe->bhqe", attn_probs.astype(jnp.bfloat16), value_heads, preferred_element_type=jnp.float32) / prob_sum
    attn_proj = jnp.einsum("cirf,ife->cre", attn_mixed.astype(jnp.bfloat16), w_out, preferred_element_type=jnp.float32).astype(jnp.bfloat16)
    return (combined.astype(jnp.float32) + attn_proj.astype(jnp.float32)).astype(jnp.bfloat16)


def combine_kernel(stages, ep_size, eo, key, gate, resid, shared, y_out,
                   t_in, t_own, w, sbuf, pbuf, rbuf, rx, ysend,
                   tab_send, tab_recv, own_sem, ring_send, ring_recv, rx_send, rx_recv, y_send, y_recv):
    micros, experts, slots_total, dim = eo.shape
    chips = ep_size // CORES
    cap = slots_total // ep_size
    half = dim // CORES
    tok = key.shape[2]
    top_k = key.shape[3]
    rows = experts * cap
    group = tok // 2

    me = lax.axis_index("ep")
    pp = lax.axis_index("pp")
    chip, core = me // CORES, me % CORES
    other = 1 - core
    partner = chip * CORES + other
    step_mine = 1 + core * (chips - 2)
    step_other = 1 + other * (chips - 2)
    nxt = ((chip + step_mine) % chips) * CORES + core
    prv = ((chip + chips - step_mine) % chips) * CORES + core
    up = (pp + 1) % stages
    down = (pp + stages - 1) % stages

    barrier = pltpu.get_barrier_semaphore()
    pl.semaphore_signal(barrier, inc=1, device_id={"ep": prv}, device_id_type=MESH)
    pl.semaphore_signal(barrier, inc=1, device_id={"ep": partner}, device_id_type=MESH)
    pl.semaphore_signal(barrier, inc=1, device_id={"pp": down}, device_id_type=MESH)
    pl.semaphore_wait(barrier, 3)

    def dest_chip(s, stride):
        return (chip + (chips - s) * stride) % chips

    def cols(which):
        return pl.ds(pl.multiple_of(which * half, 128), half)

    def table_copy(micro, s, j):
        dest = dest_chip(s, step_other) * CORES + (other + j) % CORES
        return pltpu.make_async_remote_copy(
            src_ref=eo.at[micro, :, pl.ds(pl.multiple_of(dest * cap, 16), cap), cols(other)],
            dst_ref=t_in.at[micro, s - 1, j],
            send_sem=tab_send.at[micro, s - 1, j],
            recv_sem=tab_recv.at[micro, s - 1, j],
            device_id={"ep": partner}, device_id_type=MESH)

    def own_copy(micro, s, j, slot):
        dest = dest_chip(s, step_mine) * CORES + (core + j) % CORES
        return pltpu.make_async_copy(
            eo.at[micro, :, pl.ds(pl.multiple_of(dest * cap, 16), cap), cols(core)],
            t_own.at[slot, j], own_sem.at[slot, j])

    units = [(m, s) for m in range(micros) for s in range(1, chips + 1)]
    for m, s in units:
        for j in range(CORES):
            table_copy(m, s, j).start()

    def load_own(u):
        m, s = units[u]
        for j in range(CORES):
            own_copy(m, s, j, u % 2).start()

    load_own(0)
    load_own(1)

    block = 16

    def partial(u, out):
        m, s = units[u]
        for j in range(CORES):
            dest = dest_chip(s, step_mine) * CORES + (core + j) % CORES

            def build(b, _):
                r0 = pl.multiple_of(b * block, block)
                keys = key[m, dest, pl.ds(r0, block), :]
                gates = gate[m, dest, pl.ds(r0, block), :]
                lane = lax.broadcasted_iota(jnp.int32, (block, rows), 1)
                for h, holder in enumerate((me, partner)):
                    local = keys - holder * rows
                    weights = jnp.zeros((block, rows), jnp.float32)
                    for choice in range(top_k):
                        weights = jnp.where(local[:, choice:choice + 1] == lane, gates[:, choice:choice + 1], weights)
                    high = jnp.minimum(weights, BF16_MAX).astype(jnp.bfloat16)
                    rest = weights - high.astype(jnp.float32)
                    mid = rest.astype(jnp.bfloat16)
                    low = (rest - mid.astype(jnp.float32)).astype(jnp.bfloat16)
                    w[h, 0, pl.ds(r0, block), :] = high
                    w[h, 1, pl.ds(r0, block), :] = mid
                    w[h, 2, pl.ds(r0, block), :] = low
                return 0

            lax.fori_loop(0, tok // block, build, 0)
            own_copy(m, s, j, u % 2).wait()
            table_copy(m, s, j).wait_recv()

            def mult(n, _):
                c0 = pl.multiple_of(n * 256, 256)
                acc = jnp.zeros((tok, 256), jnp.float32)
                for h in range(2):
                    table = t_own.at[u % 2, j] if h == 0 else t_in.at[m, s - 1, j]
                    block_rows = table[:, :, pl.ds(c0, 256)].reshape(rows, 256)
                    for part in range(3):
                        acc += jnp.dot(w[h, part], block_rows, preferred_element_type=jnp.float32)
                for grp in range(2):
                    out[grp, j, :, pl.ds(c0, 256)] = acc[grp * group:(grp + 1) * group]
                return 0

            lax.fori_loop(0, half // 256, mult, 0)
        if u + 2 < len(units):
            load_own(u + 2)

    def ring_copy(m, s, grp):
        src = sbuf.at[m, grp] if s == 1 else rbuf.at[m, s - 2, grp]
        return pltpu.make_async_remote_copy(
            src_ref=src, dst_ref=rbuf.at[m, s - 1, grp],
            send_sem=ring_send.at[m, s - 1, grp], recv_sem=ring_recv.at[m, s - 1, grp],
            device_id={"ep": nxt}, device_id_type=MESH)

    def add_in(m, s, grp, slot):
        def body(b, _):
            r0 = pl.multiple_of(b * 8, 8)
            for j in range(CORES):
                rbuf[m, s - 1, grp, j, pl.ds(r0, 8), :] += pbuf[slot, grp, j, pl.ds(r0, 8), :]
            return 0
        lax.fori_loop(0, group // 8, body, 0)

    def pass_on(m, s, slot):
        for grp in range(2):
            ring_copy(m, s, grp).wait_recv()
            add_in(m, s, grp, slot)
            ring_copy(m, s + 1, grp).start()

    def rx_copy(m, grp):
        return pltpu.make_async_remote_copy(
            src_ref=rbuf.at[m, chips - 2, grp, 1], dst_ref=rx.at[m, grp],
            send_sem=rx_send.at[m, grp], recv_sem=rx_recv.at[m, grp],
            device_id={"ep": partner}, device_id_type=MESH)

    def y_copy(m, grp):
        return pltpu.make_async_remote_copy(
            src_ref=ysend.at[m, grp], dst_ref=y_out.at[m, grp],
            send_sem=y_send.at[m, grp], recv_sem=y_recv.at[m, grp],
            device_id={"pp": up}, device_id_type=MESH)

    def finish(m, slot):
        for grp in range(2):
            ring_copy(m, chips - 1, grp).wait_recv()
            add_in(m, chips - 1, grp, slot)
            rx_copy(m, grp).start()
        for grp in range(2):
            rx_copy(m, grp).wait_recv()

            def body(b, _):
                r0 = pl.multiple_of(b * 16, 16)
                for which, sums in ((core, rbuf.at[m, chips - 2, grp, 0]), (other, rx.at[m, grp])):
                    base = resid[m, grp, pl.ds(r0, 16), cols(which)].astype(jnp.float32)
                    base = base + shared[m, grp, pl.ds(r0, 16), cols(which)].astype(jnp.float32)
                    ysend[m, grp, pl.ds(r0, 16), cols(which)] = (base + sums[pl.ds(r0, 16), :]).astype(jnp.bfloat16)
                return 0

            lax.fori_loop(0, group // 16, body, 0)
            y_copy(m, grp).start()

    def send_first(m):
        for grp in range(2):
            ring_copy(m, 1, grp).start()

    partial(0, sbuf.at[0])
    send_first(0)
    partial(1, pbuf.at[0])
    partial(2, pbuf.at[1])
    pass_on(0, 1, 0)
    partial(3, pbuf.at[0])
    partial(4, sbuf.at[1])
    pass_on(0, 2, 1)
    send_first(1)
    partial(5, pbuf.at[1])
    finish(0, 0)
    partial(6, pbuf.at[0])
    pass_on(1, 1, 1)
    partial(7, pbuf.at[1])
    pass_on(1, 2, 0)
    finish(1, 1)

    for m, s in units:
        for j in range(CORES):
            table_copy(m, s, j).wait_send()
    for m in range(micros):
        for grp in range(2):
            for s in range(1, chips):
                ring_copy(m, s, grp).wait_send()
            rx_copy(m, grp).wait_send()
            y_copy(m, grp).wait()


def solution(mesh):
    stages = mesh.shape["pp"]
    ep_size = mesh.shape["ep"]
    tok_spec = P("pp", "data", "ep", None, None)
    vec_spec = P("pp", None)
    mat_spec = P("pp", None, None)
    head_spec = P("pp", None, None, None)

    def device_step(expert_out, expert_ids, slot_ids, gate_weights, residual, norm_moe, w_gate, w_up, w_down, norm_attn, w_query, w_key, w_value, w_out):
        micros, experts, slots_total, dim = expert_out.shape[1:]
        cap = slots_total // ep_size
        chips = ep_size // CORES
        half = dim // CORES
        seqs, seq_len, top_k = expert_ids.shape[2:]
        tok = seqs * seq_len
        group = tok // 2
        first_slot = lax.axis_index("ep") * cap
        slot_here = slot_ids[0].reshape(micros, tok, top_k)
        key = jnp.where(slot_here >= 0, expert_ids[0].reshape(micros, tok, top_k) * cap + slot_here - first_slot, -1)
        key = lax.all_gather(key, "ep", axis=1)
        gate = lax.all_gather(gate_weights[0].reshape(micros, tok, top_k), "ep", axis=1)
        resid = residual[0].reshape(micros * seqs, seq_len, dim)
        shared = shared_expert(resid, norm_moe[0], w_gate[0], w_up[0], w_down[0])
        vmem = pl.BlockSpec(memory_space=pltpu.VMEM)
        anyspace = pl.BlockSpec(memory_space=pl.ANY)
        incoming = pl.pallas_call(
            functools.partial(combine_kernel, stages, ep_size),
            out_shape=jax.ShapeDtypeStruct((micros, 2, group, dim), jnp.bfloat16),
            in_specs=[anyspace, vmem, vmem, vmem, vmem],
            out_specs=anyspace,
            scratch_shapes=[
                pltpu.VMEM((micros, chips, CORES, experts, cap, half), jnp.bfloat16),
                pltpu.VMEM((2, CORES, experts, cap, half), jnp.bfloat16),
                pltpu.VMEM((2, 3, tok, experts * cap), jnp.bfloat16),
                pltpu.VMEM((micros, 2, CORES, group, half), jnp.float32),
                pltpu.VMEM((2, 2, CORES, group, half), jnp.float32),
                pltpu.VMEM((micros, chips - 1, 2, CORES, group, half), jnp.float32),
                pltpu.VMEM((micros, 2, group, half), jnp.float32),
                pltpu.VMEM((micros, 2, group, dim), jnp.bfloat16),
                pltpu.SemaphoreType.DMA((micros, chips, CORES)),
                pltpu.SemaphoreType.DMA((micros, chips, CORES)),
                pltpu.SemaphoreType.DMA((2, CORES)),
                pltpu.SemaphoreType.DMA((micros, chips - 1, 2)),
                pltpu.SemaphoreType.DMA((micros, chips - 1, 2)),
                pltpu.SemaphoreType.DMA((micros, 2)),
                pltpu.SemaphoreType.DMA((micros, 2)),
                pltpu.SemaphoreType.DMA((micros, 2)),
                pltpu.SemaphoreType.DMA((micros, 2)),
            ],
            compiler_params=pltpu.CompilerParams(collective_id=0, has_side_effects=True, vmem_limit_bytes=66_000_000),
            cost_estimate=pl.CostEstimate(flops=30_000_000_000, bytes_accessed=64_000_000, transcendentals=0),
        )(expert_out[0], key, gate, residual[0].reshape(micros, 2, group, dim), shared.reshape(micros, 2, group, dim))
        out = attention_block(incoming.reshape(micros * seqs, seq_len, dim), norm_attn[0], w_query[0], w_key[0], w_value[0], w_out[0])
        return out.reshape(1, micros, seqs, seq_len, dim)

    in_specs = (tok_spec,) * 5 + (vec_spec, mat_spec, mat_spec, mat_spec, vec_spec, head_spec, head_spec, head_spec, head_spec)
    return jax.shard_map(device_step, mesh=mesh, in_specs=in_specs, out_specs=tok_spec, check_vma=False)
```

```python
import functools
import math
import jax
import jax.numpy as jnp
from jax import lax
from jax.experimental import pallas as pl
from jax.experimental.pallas import tpu as pltpu
from jax.sharding import PartitionSpec as P

EPSILON = 1e-6
CORES = 2
PARTS = 3
GROUPS = 2
MESH = pl.DeviceIdType.MESH
BF16_MAX = 3.3895313892515355e38
F32 = jnp.float32
BF16 = jnp.bfloat16


def dot(a, b):
    return jnp.dot(a, b, preferred_element_type=F32)


def boundary_kernel(stages, ep_size, seq_len,
                    eo, ids, slots, gates, resid, norm_moe, w_gate, w_up, w_down, norm_attn, w_query, w_key, w_value, w_out,
                    out, w_heads,
                    t_in, t_own, w, sbuf, pbuf, rbuf, rx, ysend, y_in, shared, pool_in, pool_out, raw, turned, xn, acc, kp, kr, kt,
                    tab_send, tab_recv, own_sem, ring_send, ring_recv, rx_send, rx_recv, y_send, y_recv,
                    key_send, key_recv, load_sem, raw_sem, turn_sem, out_sem, free_sem):
    micros, experts, slots_total, dim = eo.shape
    chips = ep_size // CORES
    cap = slots_total // ep_size
    half = dim // CORES
    top_k = ids.shape[2]
    group = rbuf.shape[4]
    tok = group * GROUPS
    seqs = group // seq_len
    rows = experts * cap
    heads, head_dim = w_query.shape[1:]
    head_groups, width = w_heads.shape[1], w_heads.shape[3]
    ff = w_gate.shape[1]

    me = lax.axis_index("ep")
    pp = lax.axis_index("pp")
    chip, core = me // CORES, me % CORES
    other = 1 - core
    partner = chip * CORES + other
    step_mine = 1 + core * (chips - 2)
    step_other = 1 + other * (chips - 2)
    nxt = ((chip + step_mine) % chips) * CORES + core
    up = (pp + 1) % stages
    down = (pp + stages - 1) % stages

    peers = [(a, b) for a in range(chips) for b in range(CORES) if (a, b) != (0, 0)]

    def peer_id(a, b):
        return ((chip + a) % chips) * CORES + (core + b) % CORES

    barrier = pltpu.get_barrier_semaphore()
    for a, b in peers:
        pl.semaphore_signal(barrier, inc=1, device_id={"ep": peer_id(a, b)}, device_id_type=MESH)
    pl.semaphore_signal(barrier, inc=1, device_id={"pp": down}, device_id_type=MESH)

    def dest_chip(s, stride):
        return (chip + (chips - s) * stride) % chips

    def cols(which):
        return pl.ds(pl.multiple_of(which * half, 128), half)

    def table_copy(m, s, j):
        dest = dest_chip(s, step_other) * CORES + (other + j) % CORES
        return pltpu.make_async_remote_copy(
            src_ref=eo.at[m, :, pl.ds(pl.multiple_of(dest * cap, 16), cap), cols(other)],
            dst_ref=t_in.at[s - 1, j], send_sem=tab_send.at[m, s - 1, j], recv_sem=tab_recv.at[m, s - 1, j],
            device_id={"ep": partner}, device_id_type=MESH)

    units = [(m, s) for m in range(micros) for s in range(1, chips + 1)]

    def own_copy(u, j):
        m, s = units[u]
        dest = dest_chip(s, step_mine) * CORES + (core + j) % CORES
        return pltpu.make_async_copy(
            eo.at[m, :, pl.ds(pl.multiple_of(dest * cap, 16), cap), cols(core)],
            t_own.at[u % 2, j], own_sem.at[u % 2, j])

    def load_own(u):
        for j in range(CORES):
            own_copy(u, j).start()

    load_own(0)
    load_own(1)

    def shared_loads():
        halves = [pl.ds(0, width), pl.ds(width, width)]
        return [
            pltpu.make_async_copy(w_gate.at[:, halves[0]], pool_in.at[0, 0], load_sem.at[0, 0]),
            pltpu.make_async_copy(w_gate.at[:, halves[1]], pool_in.at[0, 1], load_sem.at[0, 1]),
            pltpu.make_async_copy(w_up.at[:, halves[0]], pool_in.at[0, 2], load_sem.at[0, 2]),
            pltpu.make_async_copy(w_up.at[:, halves[1]], pool_in.at[1, 0], load_sem.at[1, 0]),
            pltpu.make_async_copy(w_down.at[halves[0]], pool_out.at[0], load_sem.at[0, 3]),
            pltpu.make_async_copy(w_down.at[halves[1]], pool_out.at[1], load_sem.at[1, 3]),
        ]

    first = me * cap
    for m in range(micros):
        for grp in range(GROUPS):
            key_rows, gate_rows = [], []
            for q in range(seqs):
                slot_here = slots[m, grp * seqs + q]
                key_here = ids[m, grp * seqs + q] * cap + (slot_here - first)
                key_rows.append(jnp.where(slot_here >= 0, key_here, -1).astype(F32))
                gate_rows.append(gates[m, grp * seqs + q])
            key_rows = jnp.concatenate(key_rows, axis=1)
            gate_rows = jnp.concatenate(gate_rows, axis=1)
            kp[m, grp, 0] = key_rows
            kp[m, grp, 1] = gate_rows
            kr[m, grp, (chips - 1) * CORES, 0] = key_rows
            kr[m, grp, (chips - 1) * CORES, 1] = gate_rows

    pl.semaphore_wait(barrier, len(peers) + 1)

    def key_copy(a, b):
        stride = 1 + ((core + b) % CORES) * (chips - 2)
        place = ((chips - 1 + a * stride) % chips) * CORES + b
        return pltpu.make_async_remote_copy(
            src_ref=kp, dst_ref=kr.at[:, :, place], send_sem=key_send.at[a, b], recv_sem=key_recv.at[place],
            device_id={"ep": peer_id(a, b)}, device_id_type=MESH)

    def key_arrival(place):
        return pltpu.make_async_remote_copy(
            src_ref=kp, dst_ref=kr.at[:, :, place], send_sem=key_send.at[0, 0], recv_sem=key_recv.at[place],
            device_id={"ep": partner}, device_id_type=MESH)

    for a, b in peers:
        key_copy(a, b).start()
    for s in range(1, chips + 1):
        for j in range(CORES):
            table_copy(0, s, j).start()
    for copy in shared_loads():
        copy.start()
    for place in range(chips * CORES):
        if place != (chips - 1) * CORES:
            key_arrival(place).wait_recv()
    for m in range(micros):
        for grp in range(GROUPS):
            kt[m, grp] = kr[m, grp].reshape(chips * CORES * 2 * top_k, group).T

    block = 32
    lane = lax.broadcasted_iota(jnp.int32, (block, rows), 1).astype(F32)

    def build_rows(v, grp, r0):
        m, s = units[v // CORES]
        base = ((s - 1) * CORES + v % CORES) * 2 * top_k
        known = kt[m, grp, pl.ds(r0, block), :]
        keys, scale = known[:, base:base + top_k], known[:, base + top_k:base + 2 * top_k]
        r1 = pl.multiple_of(grp * group + r0, block)
        for h, holder in enumerate((me, partner)):
            local = keys - (holder * rows).astype(F32)
            weights = jnp.zeros((block, rows), F32)
            for choice in range(top_k):
                weights = jnp.where(local[:, choice:choice + 1] == lane, scale[:, choice:choice + 1], weights)
            high = jnp.minimum(weights, BF16_MAX).astype(BF16)
            rest = weights - high.astype(F32)
            mid = rest.astype(BF16)
            low = (rest - mid.astype(F32)).astype(BF16)
            for part, value in enumerate((high, mid, low)):
                w[v % 2, h, part, pl.ds(r1, block), :] = value

    pieces = half // width

    def step(v, target):
        u, j = v // CORES, v % CORES
        m, s = units[u]
        own_copy(u, j).wait()
        table_copy(m, s, j).wait_recv()
        span = tok // pieces

        def body(n, _):
            c0 = pl.multiple_of(n * width, width)
            total = None
            for h in range(2):
                table = (t_own.at[u % 2, j] if h == 0 else t_in.at[s - 1, j])[:, :, pl.ds(c0, width)].reshape(rows, width)
                for part in range(PARTS):
                    term = dot(w[v % 2, h, part], table)
                    total = term if total is None else total + term
            for grp in range(GROUPS):
                target[grp, j, :, pl.ds(c0, width)] = total[grp * group:(grp + 1) * group]
            if v + 1 < len(units) * CORES:
                for b in range(span // block):
                    row = n * span + b * block
                    build_rows(v + 1, row // group, pl.multiple_of(row % group, block))
            return 0

        lax.fori_loop(0, pieces, body, 0)
        if j == CORES - 1:
            if u + 2 < len(units):
                load_own(u + 2)
            if m == 0:
                pl.semaphore_signal(free_sem.at[s - 1], inc=1, device_id={"ep": partner}, device_id_type=MESH)

    def next_tables(s):
        pl.semaphore_wait(free_sem.at[s - 1], 1)
        for j in range(CORES):
            table_copy(1, s, j).start()

    def ring_copy(m, s, grp, j, q):
        part = pl.ds(q * seq_len, seq_len)
        src = sbuf.at[grp, j, part] if s == 1 else rbuf.at[m, s - 2, grp, j, part]
        return pltpu.make_async_remote_copy(
            src_ref=src, dst_ref=rbuf.at[m, s - 1, grp, j, part],
            send_sem=ring_send.at[m, s - 1, grp, j, q], recv_sem=ring_recv.at[m, s - 1, grp, j, q],
            device_id={"ep": nxt}, device_id_type=MESH)

    def send_first(m, j):
        for grp in range(GROUPS):
            for q in range(seqs):
                ring_copy(m, 1, grp, j, q).start()

    def add_in(m, s, grp, j, q, slot):
        for b in range(seq_len // block):
            part = pl.ds(q * seq_len + b * block, block)
            rbuf[m, s - 1, grp, j, part, :] += pbuf[slot, grp, j, part, :]

    def rx_copy(m, grp, q):
        part = pl.ds(q * seq_len, seq_len)
        return pltpu.make_async_remote_copy(
            src_ref=rbuf.at[m, chips - 2, grp, 1, part], dst_ref=rx.at[m, grp, part],
            send_sem=rx_send.at[m, grp, q], recv_sem=rx_recv.at[m, grp, q],
            device_id={"ep": partner}, device_id_type=MESH)

    def arrive(m, s, grp, slot):
        for q in range(seqs):
            for j in (1, 0):
                ring_copy(m, s, grp, j, q).wait_recv()
                add_in(m, s, grp, j, q, slot)
                if s < chips - 1:
                    ring_copy(m, s + 1, grp, j, q).start()
                elif j == 1:
                    rx_copy(m, grp, q).start()

    def y_copy(m, grp, q):
        part = pl.ds(q * seq_len, seq_len)
        return pltpu.make_async_remote_copy(
            src_ref=ysend.at[grp, part], dst_ref=y_in.at[m, pl.ds(grp * group + q * seq_len, seq_len)],
            send_sem=y_send.at[m, grp, q], recv_sem=y_recv.at[m, grp, q],
            device_id={"pp": up}, device_id_type=MESH)

    def combine(m, grp):
        for q in range(seqs):
            if m > 0:
                y_copy(m - 1, grp, q).wait_send()
            rx_copy(m, grp, q).wait_recv()

            def body(b, _):
                r0 = pl.multiple_of(q * seq_len + b * 16, 16)
                r1 = pl.multiple_of(m * tok + grp * group + r0, 16)
                for which, sums in ((core, rbuf.at[m, chips - 2, grp, 0]), (other, rx.at[m, grp])):
                    base = resid[pl.ds(r1, 16), cols(which)].astype(F32) + shared[pl.ds(r1, 16), cols(which)].astype(F32)
                    ysend[grp, pl.ds(r0, 16), cols(which)] = (base + sums[pl.ds(r0, 16), :]).astype(BF16)
                return 0

            lax.fori_loop(0, seq_len // 16, body, 0)
            y_copy(m, grp, q).start()

    def normalize(source, base, count, gain):
        def body(b, _):
            r0 = pl.multiple_of(b * 16, 16)
            values = source[pl.ds(pl.multiple_of(base + r0, 16), 16), :].astype(F32)
            inv_rms = lax.rsqrt(jnp.mean(values * values, axis=-1, keepdims=True) + EPSILON)
            xn[pl.ds(r0, 16), :] = (values * inv_rms * gain[...]).astype(BF16)
            return 0
        lax.fori_loop(0, count // 16, body, 0)

    def shared_expert():
        for copy in shared_loads():
            copy.wait()
        gate_refs = (pool_in.at[0, 0], pool_in.at[0, 1])
        up_refs = (pool_in.at[0, 2], pool_in.at[1, 0])

        def body(m, _):
            normalize(resid, m * tok, tok, norm_moe)
            hidden = []
            for f in range(ff // width):
                gate_act = dot(xn[...], gate_refs[f][...])
                up_act = dot(xn[...], up_refs[f][...])
                hidden.append((gate_act * jax.nn.sigmoid(gate_act) * up_act).astype(BF16))
            r0 = pl.multiple_of(m * tok, 16)
            for n in range(dim // (2 * width)):
                span = pl.ds(n * 2 * width, 2 * width)
                total = dot(hidden[0], pool_out[0, :, span]) + dot(hidden[1], pool_out[1, :, span])
                shared[pl.ds(r0, tok), span] = total.astype(BF16)
            return 0

        lax.fori_loop(0, micros, body, 0)

    chunk = raw.shape[1]

    def to_head_groups(kind, source):
        count = dim // chunk

        def fetch(c):
            return pltpu.make_async_copy(source.at[pl.ds(pl.multiple_of(c * chunk, chunk), chunk)], raw.at[c % 2], raw_sem.at[c % 2])

        def flush(c):
            return pltpu.make_async_copy(turned.at[c % 2], w_heads.at[kind, :, pl.ds(pl.multiple_of(c * chunk, chunk), chunk)], turn_sem.at[c % 2])

        fetch(0).start()

        def body(c, _):
            @pl.when(c + 1 < count)
            def _():
                fetch(c + 1).start()
            fetch(c).wait()

            @pl.when(c >= 2)
            def _():
                flush(c - 2).wait()

            def turn(b, _):
                r0 = pl.multiple_of(b * 32, 32)
                value = jnp.swapaxes(raw[c % 2, pl.ds(r0, 32)], 0, 1)
                for h in range(heads):
                    place = (h * head_dim) % width
                    turned[c % 2, h * head_dim // width, pl.ds(r0, 32), place:place + head_dim] = value[h]
                return 0

            lax.fori_loop(0, chunk // 32, turn, 0)
            flush(c).start()
            return 0

        lax.fori_loop(0, count, body, 0)
        flush(count - 2).wait()
        flush(count - 1).wait()

    def weight_loads(g, slot):
        loads = [pltpu.make_async_copy(w_heads.at[kind, g], pool_in.at[slot, kind], load_sem.at[slot, kind]) for kind in range(3)]
        loads.append(pltpu.make_async_copy(w_out.at[pl.ds(pl.multiple_of(g * width, width), width)], pool_out.at[slot], load_sem.at[slot, 3]))
        return loads

    def prefetch():
        for g in range(2):
            for copy in weight_loads(g, g):
                copy.start()

    span_q = 128
    score_scale = 1.0 / math.sqrt(head_dim)

    def attend(g0, g1):
        row = lax.broadcasted_iota(jnp.int32, (span_q, span_q), 0)
        col = lax.broadcasted_iota(jnp.int32, (span_q, span_q), 1)
        visible = (row >= col) & (row // seq_len == col // seq_len)

        def body(g, _):
            slot = g % 2
            for copy in weight_loads(g, slot):
                copy.wait()
            queries = dot(xn[...], pool_in[slot, 0]).astype(BF16)
            key_heads = dot(xn[...], pool_in[slot, 1]).astype(BF16)
            value_heads = dot(xn[...], pool_in[slot, 2]).astype(BF16)
            mixed = []
            for r in range(tok // span_q):
                line = []
                for h in range(width // head_dim):
                    part = (slice(r * span_q, (r + 1) * span_q), slice(h * head_dim, (h + 1) * head_dim))
                    scores = lax.dot_general(queries[part], key_heads[part], (((1,), (1,)), ((), ())), preferred_element_type=F32) * score_scale
                    scores = jnp.where(visible, scores, -1e30)
                    probs = jnp.exp(scores - jnp.max(scores, axis=-1, keepdims=True))
                    total = jnp.sum(probs, axis=-1, keepdims=True)
                    line.append((dot(probs.astype(BF16), value_heads[part]) / total).astype(BF16))
                mixed.append(jnp.concatenate(line, axis=1))
            mixed = jnp.concatenate(mixed, axis=0)
            for n in range(dim // (2 * width)):
                span = pl.ds(n * 2 * width, 2 * width)
                acc[:, span] += dot(mixed, pool_out[slot, :, span])

            @pl.when(g + 2 < head_groups)
            def _():
                for copy in weight_loads(g + 2, slot):
                    copy.start()
            return 0

        lax.fori_loop(g0, g1, body, 0)

    def out_copy(m):
        return pltpu.make_async_copy(xn, out.at[m], out_sem.at[m])

    def begin_attention(m):
        for grp in range(GROUPS):
            for q in range(seqs):
                y_copy(m, grp, q).wait_recv()
        if m > 0:
            out_copy(m - 1).wait()
        normalize(y_in.at[m], 0, tok, norm_attn)

        def clear(b, _):
            acc[pl.ds(pl.multiple_of(b * 16, 16), 16), :] = jnp.zeros((16, dim), F32)
            return 0

        lax.fori_loop(0, tok // 16, clear, 0)

    def end_attention(m):
        def body(b, _):
            r0 = pl.multiple_of(b * 16, 16)
            proj = acc[pl.ds(r0, 16), :].astype(BF16).astype(F32)
            xn[pl.ds(r0, 16), :] = (y_in[m, pl.ds(r0, 16), :].astype(F32) + proj).astype(BF16)
            return 0
        lax.fori_loop(0, tok // 16, body, 0)
        out_copy(m).start()

    def first_rows(b, _):
        row = b * block
        build_rows(0, row // group, pl.multiple_of(row % group, block))
        return 0

    lax.fori_loop(0, tok // block, first_rows, 0)
    for j in range(CORES):
        step(j, sbuf)
        send_first(0, j)
    step(2, pbuf.at[0])
    step(3, pbuf.at[0])
    shared_expert()
    arrive(0, 1, 0, 0)
    next_tables(1)
    step(4, pbuf.at[1])
    step(5, pbuf.at[1])
    arrive(0, 1, 1, 0)
    next_tables(2)
    to_head_groups(0, w_query)
    step(6, pbuf.at[0])
    step(7, pbuf.at[0])
    arrive(0, 2, 0, 1)
    next_tables(3)
    for grp in range(GROUPS):
        for j in range(CORES):
            for q in range(seqs):
                ring_copy(0, 1, grp, j, q).wait_send()
    step(8, sbuf)
    step(9, sbuf)
    to_head_groups(1, w_key)
    arrive(0, 2, 1, 1)
    next_tables(4)
    for j in range(CORES):
        send_first(1, j)
    step(10, pbuf.at[1])
    step(11, pbuf.at[1])
    arrive(0, 3, 0, 0)
    to_head_groups(2, w_value)
    prefetch()
    combine(0, 0)
    arrive(0, 3, 1, 0)
    step(12, pbuf.at[0])
    combine(0, 1)
    step(13, pbuf.at[0])
    arrive(1, 1, 0, 1)
    begin_attention(0)
    attend(0, 4)
    arrive(1, 1, 1, 1)
    step(14, pbuf.at[1])
    step(15, pbuf.at[1])
    arrive(1, 2, 0, 0)
    attend(4, 8)
    end_attention(0)
    prefetch()
    arrive(1, 2, 1, 0)
    arrive(1, 3, 0, 1)
    combine(1, 0)
    arrive(1, 3, 1, 1)
    combine(1, 1)
    begin_attention(1)
    attend(0, 8)
    end_attention(1)
    out_copy(1).wait()

    for a, b in peers:
        key_copy(a, b).wait_send()
    for m, s in units:
        for j in range(CORES):
            table_copy(m, s, j).wait_send()
    for m in range(micros):
        for grp in range(GROUPS):
            for q in range(seqs):
                for s in range(1, chips):
                    for j in range(CORES):
                        if (m, s) != (0, 1):
                            ring_copy(m, s, grp, j, q).wait_send()
                rx_copy(m, grp, q).wait_send()
                if m == micros - 1:
                    y_copy(m, grp, q).wait_send()


def solution(mesh):
    stages = mesh.shape["pp"]
    ep_size = mesh.shape["ep"]
    tok_spec = P("pp", "data", "ep", None, None)
    vec_spec = P("pp", None)
    mat_spec = P("pp", None, None)
    head_spec = P("pp", None, None, None)

    def device_step(expert_out, expert_ids, slot_ids, gate_weights, residual, norm_moe, w_gate, w_up, w_down, norm_attn, w_query, w_key, w_value, w_out):
        micros, experts, slots_total, dim = expert_out.shape[1:]
        heads, head_dim = w_query.shape[2:]
        cap = slots_total // ep_size
        chips = ep_size // CORES
        half = dim // CORES
        seqs, seq_len, top_k = expert_ids.shape[2:]
        tok = seqs * seq_len
        group = tok // GROUPS
        width = 2 * head_dim
        head_groups = heads * head_dim // width

        def by_lane(x):
            return jnp.swapaxes(x[0], -1, -2)

        vmem = pl.BlockSpec(memory_space=pltpu.VMEM)
        anyspace = pl.BlockSpec(memory_space=pl.ANY)
        dma = pltpu.SemaphoreType.DMA
        out, _ = pl.pallas_call(
            functools.partial(boundary_kernel, stages, ep_size, seq_len),
            out_shape=[
                jax.ShapeDtypeStruct((micros, tok, dim), BF16),
                jax.ShapeDtypeStruct((3, head_groups, dim, width), BF16),
            ],
            in_specs=[anyspace, vmem, vmem, vmem, vmem, vmem, anyspace, anyspace, anyspace, vmem, anyspace, anyspace, anyspace, anyspace],
            out_specs=[anyspace, anyspace],
            scratch_shapes=[
                pltpu.VMEM((chips, CORES, experts, cap, half), BF16),
                pltpu.VMEM((2, CORES, experts, cap, half), BF16),
                pltpu.VMEM((2, 2, PARTS, tok, experts * cap), BF16),
                pltpu.VMEM((GROUPS, CORES, group, half), F32),
                pltpu.VMEM((2, GROUPS, CORES, group, half), F32),
                pltpu.VMEM((micros, chips - 1, GROUPS, CORES, group, half), F32),
                pltpu.VMEM((micros, GROUPS, group, half), F32),
                pltpu.VMEM((GROUPS, group, dim), BF16),
                pltpu.VMEM((micros, tok, dim), BF16),
                pltpu.VMEM((micros * tok, dim), BF16),
                pltpu.VMEM((2, 3, dim, width), BF16),
                pltpu.VMEM((2, width, dim), BF16),
                pltpu.VMEM((2, 256, heads, head_dim), BF16),
                pltpu.VMEM((2, head_groups, 256, width), BF16),
                pltpu.VMEM((tok, dim), BF16),
                pltpu.VMEM((tok, dim), F32),
                pltpu.VMEM((micros, GROUPS, 2, top_k, group), F32),
                pltpu.VMEM((micros, GROUPS, chips * CORES, 2, top_k, group), F32),
                pltpu.VMEM((micros, GROUPS, group, chips * CORES * 2 * top_k), F32),
                dma((micros, chips, CORES)), dma((micros, chips, CORES)), dma((2, CORES)),
                dma((micros, chips - 1, GROUPS, CORES, seqs // GROUPS)), dma((micros, chips - 1, GROUPS, CORES, seqs // GROUPS)),
                dma((micros, GROUPS, seqs // GROUPS)), dma((micros, GROUPS, seqs // GROUPS)),
                dma((micros, GROUPS, seqs // GROUPS)), dma((micros, GROUPS, seqs // GROUPS)),
                dma((chips, CORES)), dma((chips * CORES,)), dma((2, 4)), dma((2,)), dma((2,)), dma((micros,)),
                pltpu.SemaphoreType.REGULAR((chips,)),
            ],
            compiler_params=pltpu.CompilerParams(collective_id=0, has_side_effects=True, vmem_limit_bytes=67_000_000),
            cost_estimate=pl.CostEstimate(flops=50_000_000_000, bytes_accessed=200_000_000, transcendentals=0),
        )(expert_out[0], by_lane(expert_ids), by_lane(slot_ids), by_lane(gate_weights), residual[0].reshape(micros * tok, dim),
          norm_moe, w_gate[0], w_up[0], w_down[0], norm_attn, w_query[0], w_key[0], w_value[0], w_out[0].reshape(heads * head_dim, dim))
        return out.reshape(1, micros, seqs, seq_len, dim)

    in_specs = (tok_spec,) * 5 + (vec_spec, mat_spec, mat_spec, mat_spec, vec_spec, head_spec, head_spec, head_spec, head_spec)
    return jax.shard_map(device_step, mesh=mesh, in_specs=in_specs, out_specs=tok_spec, check_vma=False)
```

```python
import functools
import math
import jax
import jax.numpy as jnp
from jax import lax
from jax.experimental import pallas as pl
from jax.experimental.pallas import tpu as pltpu
from jax.sharding import PartitionSpec as P

EPSILON = 1e-6
CORES = 2
PARTS = 3
GROUPS = 2
MESH = pl.DeviceIdType.MESH
BF16_MAX = 3.3895313892515355e38
F32 = jnp.float32
BF16 = jnp.bfloat16


def dot(a, b):
    return jnp.dot(a, b, preferred_element_type=F32)


def boundary_kernel(stages, ep_size, seq_len,
                    eo, ids, slots, gates, resid, norm_moe, w_gate, w_up, w_down, norm_attn, w_query, w_key, w_value, w_out,
                    out, w_heads,
                    t_in, t_own, w, sbuf, pbuf, rbuf, rx, ysend, y_in, shared, pool_in, pool_out, raw, turned, xn, acc, qkv, mixed, kp, kr, kt,
                    tab_send, tab_recv, own_sem, ring_send, ring_recv, rx_send, rx_recv, y_send, y_recv,
                    key_send, key_recv, load_sem, raw_sem, turn_sem, out_sem, free_sem):
    micros, experts, slots_total, dim = eo.shape
    chips = ep_size // CORES
    cap = slots_total // ep_size
    half = dim // CORES
    top_k = ids.shape[2]
    group = rbuf.shape[4]
    tok = group * GROUPS
    seqs = group // seq_len
    rows = experts * cap
    heads, head_dim = w_query.shape[1:]
    head_groups, width = w_heads.shape[1], w_heads.shape[3]
    ff = w_gate.shape[1]

    me = lax.axis_index("ep")
    pp = lax.axis_index("pp")
    chip, core = me // CORES, me % CORES
    other = 1 - core
    partner = chip * CORES + other
    step_mine = 1 + core * (chips - 2)
    step_other = 1 + other * (chips - 2)
    nxt = ((chip + step_mine) % chips) * CORES + core
    up = (pp + 1) % stages
    down = (pp + stages - 1) % stages

    peers = [(s, b) for s in range(1, chips + 1) for b in range(CORES) if (s, b) != (chips, 0)]

    def peer_id(s, b):
        there = (core + b) % CORES
        return ((chip + s * (1 + there * (chips - 2))) % chips) * CORES + there

    barrier = pltpu.get_barrier_semaphore()
    for s, b in peers:
        pl.semaphore_signal(barrier, inc=1, device_id={"ep": peer_id(s, b)}, device_id_type=MESH)
    pl.semaphore_signal(barrier, inc=1, device_id={"pp": down}, device_id_type=MESH)

    def dest_chip(s, stride):
        return (chip + (chips - s) * stride) % chips

    def cols(which):
        return pl.ds(pl.multiple_of(which * half, 128), half)

    def table_copy(m, s, j):
        dest = dest_chip(s, step_other) * CORES + (other + j) % CORES
        return pltpu.make_async_remote_copy(
            src_ref=eo.at[m, :, pl.ds(pl.multiple_of(dest * cap, 16), cap), cols(other)],
            dst_ref=t_in.at[s - 1, j], send_sem=tab_send.at[m, s - 1, j], recv_sem=tab_recv.at[m, s - 1, j],
            device_id={"ep": partner}, device_id_type=MESH)

    units = [(m, s) for m in range(micros) for s in range(1, chips + 1)]

    def own_copy(u, j):
        m, s = units[u]
        dest = dest_chip(s, step_mine) * CORES + (core + j) % CORES
        return pltpu.make_async_copy(
            eo.at[m, :, pl.ds(pl.multiple_of(dest * cap, 16), cap), cols(core)],
            t_own.at[u % 2, j], own_sem.at[u % 2, j])

    def load_own(u):
        for j in range(CORES):
            own_copy(u, j).start()

    load_own(0)
    load_own(1)

    def shared_loads():
        halves = [pl.ds(0, width), pl.ds(width, width)]
        return [
            pltpu.make_async_copy(w_gate.at[:, halves[0]], pool_in.at[0, 0], load_sem.at[0, 0]),
            pltpu.make_async_copy(w_gate.at[:, halves[1]], pool_in.at[0, 1], load_sem.at[0, 1]),
            pltpu.make_async_copy(w_up.at[:, halves[0]], pool_in.at[0, 2], load_sem.at[0, 2]),
            pltpu.make_async_copy(w_up.at[:, halves[1]], pool_in.at[1, 0], load_sem.at[1, 0]),
            pltpu.make_async_copy(w_down.at[halves[0]], pool_out.at[0], load_sem.at[0, 3]),
            pltpu.make_async_copy(w_down.at[halves[1]], pool_out.at[1], load_sem.at[1, 3]),
        ]

    first = me * cap
    for m in range(micros):
        for grp in range(GROUPS):
            packed, gate_rows = [], []
            for q in range(seqs):
                slot_here = slots[m, grp * seqs + q]
                key_here = ids[m, grp * seqs + q] * cap + (slot_here - first)
                packed.append(jnp.where(slot_here >= 0, key_here, -1).astype(F32))
                gate_rows.append(gates[m, grp * seqs + q])
            packed = jnp.concatenate(packed, axis=1)
            gate_rows = jnp.concatenate(gate_rows, axis=1)
            kp[m, grp, 0] = packed
            kp[m, grp, 1] = gate_rows
            kr[m, grp, (chips - 1) * CORES, 0] = packed
            kr[m, grp, (chips - 1) * CORES, 1] = gate_rows

    with jax.named_scope("barrier"):
        pl.semaphore_wait(barrier, len(peers) + 1)

    def key_copy(m, s, b):
        place = (s - 1) * CORES + b
        return pltpu.make_async_remote_copy(
            src_ref=kp.at[m], dst_ref=kr.at[m, :, place], send_sem=key_send.at[m, s - 1, b], recv_sem=key_recv.at[m, s - 1, b],
            device_id={"ep": peer_id(s, b)}, device_id_type=MESH)

    for m in range(micros):
        for s, b in peers:
            key_copy(m, s, b).start()
    for s in range(1, chips + 1):
        for j in range(CORES):
            table_copy(0, s, j).start()
    for copy in shared_loads():
        copy.start()

    key_rows = CORES * 2 * top_k

    def take_keys(m, s):
        for b in range(CORES):
            if (s, b) in peers:
                key_copy(m, s, b).wait_recv()
        for grp in range(GROUPS):
            arrived = kr[m, grp, (s - 1) * CORES:s * CORES].reshape(key_rows, group)
            kt[m, grp, :, (s - 1) * key_rows:s * key_rows] = arrived.T

    block = 32
    lane = lax.broadcasted_iota(jnp.int32, (block, rows), 1).astype(F32)

    def build_rows(v, grp, r0):
        m, s = units[v // CORES]
        base = ((s - 1) * CORES + v % CORES) * 2 * top_k
        known = kt[m, grp, pl.ds(r0, block), :]
        keys, scale = known[:, base:base + top_k], known[:, base + top_k:base + 2 * top_k]
        r1 = pl.multiple_of(grp * group + r0, block)
        for h, holder in enumerate((me, partner)):
            local = keys - (holder * rows).astype(F32)
            weights = jnp.zeros((block, rows), F32)
            for choice in range(top_k):
                weights = jnp.where(local[:, choice:choice + 1] == lane, scale[:, choice:choice + 1], weights)
            high = jnp.minimum(weights, BF16_MAX).astype(BF16)
            rest = weights - high.astype(F32)
            mid = rest.astype(BF16)
            low = (rest - mid.astype(F32)).astype(BF16)
            for part, value in enumerate((high, mid, low)):
                w[v % 2, h, part, pl.ds(r1, block), :] = value

    pieces = half // width
    subs = len(units) * CORES

    def step(v, target, groups, following):
        u, j = v // CORES, v % CORES
        m, s = units[u]
        if groups[0] == 0:
            own_copy(u, j).wait()
            table_copy(m, s, j).wait_recv()
        r0, count = groups[0] * group, len(groups) * group
        builds = [(w_next, grp, b) for w_next, grp in following for b in range(group // block)]
        per = -(-len(builds) // pieces)

        def body(n, _):
            c0 = pl.multiple_of(n * width, width)
            total = None
            for h in range(2):
                table = (t_own.at[u % 2, j] if h == 0 else t_in.at[s - 1, j])[:, :, pl.ds(c0, width)].reshape(rows, width)
                for part in range(PARTS):
                    term = dot(w[v % 2, h, part, r0:r0 + count], table)
                    total = term if total is None else total + term
            for i, grp in enumerate(groups):
                target[grp, j, :, pl.ds(c0, width)] = total[i * group:(i + 1) * group]
            for b in range(per):
                row = (n * per + b) * block
                if len(following) == 1:
                    build_rows(following[0][0], following[0][1], pl.multiple_of(row, block))
                elif following:
                    build_rows(following[0][0], row // group, pl.multiple_of(row % group, block))
            return 0

        lax.fori_loop(0, pieces, body, 0)
        if j == CORES - 1 and groups[-1] == GROUPS - 1:
            if u + 2 < len(units):
                load_own(u + 2)
            if m == 0:
                pl.semaphore_signal(free_sem.at[s - 1], inc=1, device_id={"ep": partner}, device_id_type=MESH)

    def whole(v, target):
        both = tuple(range(GROUPS))
        with jax.named_scope("step"):
            step(v, target, both, [(v + 1, grp) for grp in both] if v + 1 < subs else [])

    def next_tables(s):
        pl.semaphore_wait(free_sem.at[s - 1], 1)
        for j in range(CORES):
            table_copy(1, s, j).start()

    def ring_copy(m, s, grp, j, q):
        part = pl.ds(q * seq_len, seq_len)
        src = sbuf.at[grp, j, part] if s == 1 else rbuf.at[m, s - 2, grp, j, part]
        return pltpu.make_async_remote_copy(
            src_ref=src, dst_ref=rbuf.at[m, s - 1, grp, j, part],
            send_sem=ring_send.at[m, s - 1, grp, j, q], recv_sem=ring_recv.at[m, s - 1, grp, j, q],
            device_id={"ep": nxt}, device_id_type=MESH)

    def send_first(m, grp, order):
        for j in order:
            for q in range(seqs):
                ring_copy(m, 1, grp, j, q).start()

    def add_in(m, s, grp, j, q, slot):
        for b in range(seq_len // block):
            part = pl.ds(q * seq_len + b * block, block)
            rbuf[m, s - 1, grp, j, part, :] += pbuf[slot, grp, j, part, :]

    def rx_copy(m, grp, q):
        part = pl.ds(q * seq_len, seq_len)
        return pltpu.make_async_remote_copy(
            src_ref=rbuf.at[m, chips - 2, grp, 1, part], dst_ref=rx.at[m, grp, part],
            send_sem=rx_send.at[m, grp, q], recv_sem=rx_recv.at[m, grp, q],
            device_id={"ep": partner}, device_id_type=MESH)

    def arrive(m, s, grp, slot):
        for q in range(seqs):
            for j in (1, 0):
                ring_copy(m, s, grp, j, q).wait_recv()
                add_in(m, s, grp, j, q, slot)
                if s < chips - 1:
                    ring_copy(m, s + 1, grp, j, q).start()
                elif j == 1:
                    rx_copy(m, grp, q).start()
            if s == chips - 1:
                combine(m, grp, q)

    def y_copy(m, grp, q):
        part = pl.ds(q * seq_len, seq_len)
        return pltpu.make_async_remote_copy(
            src_ref=ysend.at[grp, part], dst_ref=y_in.at[m, pl.ds(grp * group + q * seq_len, seq_len)],
            send_sem=y_send.at[m, grp, q], recv_sem=y_recv.at[m, grp, q],
            device_id={"pp": up}, device_id_type=MESH)

    def combine(m, grp, q):
        if m > 0:
            y_copy(m - 1, grp, q).wait_send()
        rx_copy(m, grp, q).wait_recv()

        def body(b, _):
            r0 = pl.multiple_of(q * seq_len + b * 16, 16)
            r1 = pl.multiple_of(m * tok + grp * group + r0, 16)
            for which, sums in ((core, rbuf.at[m, chips - 2, grp, 0]), (other, rx.at[m, grp])):
                base = resid[pl.ds(r1, 16), cols(which)].astype(F32) + shared[pl.ds(r1, 16), cols(which)].astype(F32)
                ysend[grp, pl.ds(r0, 16), cols(which)] = (base + sums[pl.ds(r0, 16), :]).astype(BF16)
            return 0

        lax.fori_loop(0, seq_len // 16, body, 0)
        y_copy(m, grp, q).start()

    def normalize(source, base, count, gain):
        def body(b, _):
            r0 = pl.multiple_of(b * 16, 16)
            values = source[pl.ds(pl.multiple_of(base + r0, 16), 16), :].astype(F32)
            inv_rms = lax.rsqrt(jnp.mean(values * values, axis=-1, keepdims=True) + EPSILON)
            xn[pl.ds(r0, 16), :] = (values * inv_rms * gain[...]).astype(BF16)
            return 0
        lax.fori_loop(0, count // 16, body, 0)

    def shared_expert():
        for copy in shared_loads():
            copy.wait()
        gate_refs = (pool_in.at[0, 0], pool_in.at[0, 1])
        up_refs = (pool_in.at[0, 2], pool_in.at[1, 0])

        def body(m, _):
            normalize(resid, m * tok, tok, norm_moe)
            hidden = []
            for f in range(ff // width):
                gate_act = dot(xn[...], gate_refs[f][...])
                up_act = dot(xn[...], up_refs[f][...])
                hidden.append((gate_act * jax.nn.sigmoid(gate_act) * up_act).astype(BF16))
            r0 = pl.multiple_of(m * tok, 16)
            for n in range(dim // (2 * width)):
                span = pl.ds(n * 2 * width, 2 * width)
                total = dot(hidden[0], pool_out[0, :, span]) + dot(hidden[1], pool_out[1, :, span])
                shared[pl.ds(r0, tok), span] = total.astype(BF16)
            return 0

        lax.fori_loop(0, micros, body, 0)

    depth, chunk = raw.shape[:2]

    def to_head_groups(kind, source):
        count = dim // chunk

        def fetch(c):
            return pltpu.make_async_copy(source.at[pl.ds(pl.multiple_of(c * chunk, chunk), chunk)], raw.at[c % depth], raw_sem.at[c % depth])

        def flush(c):
            return pltpu.make_async_copy(turned.at[c % depth], w_heads.at[kind, :, pl.ds(pl.multiple_of(c * chunk, chunk), chunk)], turn_sem.at[c % depth])

        for c in range(depth - 1):
            fetch(c).start()

        def body(c, _):
            @pl.when(c + depth - 1 < count)
            def _():
                fetch(c + depth - 1).start()
            fetch(c).wait()

            @pl.when(c >= depth)
            def _():
                flush(c - depth).wait()

            def turn(b, _):
                r0 = pl.multiple_of(b * 32, 32)
                value = jnp.swapaxes(raw[c % depth, pl.ds(r0, 32)], 0, 1)
                for h in range(heads):
                    place = (h * head_dim) % width
                    turned[c % depth, h * head_dim // width, pl.ds(r0, 32), place:place + head_dim] = value[h]
                return 0

            lax.fori_loop(0, chunk // 32, turn, 0)
            flush(c).start()
            return 0

        with jax.named_scope("rewrite"):
            lax.fori_loop(0, count, body, 0)
            for c in range(count - depth, count):
                flush(c).wait()

    def in_loads(g, slot):
        return [pltpu.make_async_copy(w_heads.at[kind, g], pool_in.at[slot, kind], load_sem.at[slot, kind]) for kind in range(3)]

    def out_load(g, slot):
        return pltpu.make_async_copy(w_out.at[pl.ds(pl.multiple_of(g * width, width), width)], pool_out.at[slot], load_sem.at[slot, 3])

    def prefetch():
        for g in range(2):
            for copy in in_loads(g, g):
                copy.start()
            out_load(g, g).start()

    span_q = 128
    score_scale = 1.0 / math.sqrt(head_dim)

    def project(g, slot):
        for kind in range(3):
            qkv[slot, kind] = dot(xn[...], pool_in[slot, kind]).astype(BF16)

    def mix(slot):
        row = lax.broadcasted_iota(jnp.int32, (span_q, span_q), 0)
        col = lax.broadcasted_iota(jnp.int32, (span_q, span_q), 1)
        visible = (row >= col) & (row // seq_len == col // seq_len)
        for r in range(tok // span_q):
            line = []
            for h in range(width // head_dim):
                part = (slice(r * span_q, (r + 1) * span_q), slice(h * head_dim, (h + 1) * head_dim))
                scores = lax.dot_general(qkv[(slot, 0) + part], qkv[(slot, 1) + part], (((1,), (1,)), ((), ())), preferred_element_type=F32) * score_scale
                scores = jnp.where(visible, scores, -1e30)
                probs = jnp.exp(scores - jnp.max(scores, axis=-1, keepdims=True))
                total = jnp.sum(probs, axis=-1, keepdims=True)
                line.append((dot(probs.astype(BF16), qkv[(slot, 2) + part]) / total).astype(BF16))
            mixed[slot, r * span_q:(r + 1) * span_q, :] = jnp.concatenate(line, axis=1)
        for n in range(dim // (2 * width)):
            span = pl.ds(n * 2 * width, 2 * width)
            acc[:, span] += dot(mixed[slot], pool_out[slot, :, span])

    def attend(g0, g1):
        def body(g, _):
            slot = g % 2
            for copy in in_loads(g, slot):
                copy.wait()
            out_load(g - 1, 1 - slot).wait()
            mix(1 - slot)
            project(g, slot)

            @pl.when(g + 2 < head_groups)
            def _():
                for copy in in_loads(g + 2, slot):
                    copy.start()

            @pl.when(g + 1 < head_groups)
            def _():
                out_load(g + 1, 1 - slot).start()
            return 0

        with jax.named_scope("attend"):
            lax.fori_loop(g0, g1, body, 0)

    def out_copy(m):
        return pltpu.make_async_copy(xn, out.at[m], out_sem.at[m])

    def begin_attention(m):
        for grp in range(GROUPS):
            for q in range(seqs):
                y_copy(m, grp, q).wait_recv()
        if m > 0:
            out_copy(m - 1).wait()
        normalize(y_in.at[m], 0, tok, norm_attn)

        def clear(b, _):
            acc[pl.ds(pl.multiple_of(b * 16, 16), 16), :] = jnp.zeros((16, dim), F32)
            return 0

        lax.fori_loop(0, tok // 16, clear, 0)
        for copy in in_loads(0, 0):
            copy.wait()
        project(0, 0)
        for copy in in_loads(2, 0):
            copy.start()

    def end_attention(m):
        out_load(head_groups - 1, 1).wait()
        mix(1)

        def body(b, _):
            r0 = pl.multiple_of(b * 16, 16)
            proj = acc[pl.ds(r0, 16), :].astype(BF16).astype(F32)
            xn[pl.ds(r0, 16), :] = (y_in[m, pl.ds(r0, 16), :].astype(F32) + proj).astype(BF16)
            return 0
        lax.fori_loop(0, tok // 16, body, 0)
        out_copy(m).start()

    def scoped(name, task, *args):
        with jax.named_scope(name):
            task(*args)

    def first_rows(b, _):
        build_rows(0, 0, pl.multiple_of(b * block, block))
        return 0

    scoped("keys", take_keys, 0, 1)
    scoped("build", lax.fori_loop, 0, group // block, first_rows, 0)
    for grp in range(GROUPS):
        for j in range(CORES):
            if (grp, j) == (1, 1):
                following = [(2, 0), (2, 1)]
            else:
                following = [((j + 1) % CORES, grp + j)]
            scoped("half", step, j, sbuf, (grp,), following)
            send_first(0, grp, (j,))
            if (grp, j) == (0, 1):
                for m, s in units[1:]:
                    scoped("keys", take_keys, m, s)
    whole(2, pbuf.at[0])
    whole(3, pbuf.at[0])
    scoped("shared", shared_expert)
    scoped("arrive", arrive, 0, 1, 0, 0)
    next_tables(1)
    to_head_groups(0, w_query)
    whole(4, pbuf.at[1])
    whole(5, pbuf.at[1])
    scoped("arrive", arrive, 0, 1, 1, 0)
    next_tables(2)
    whole(6, pbuf.at[0])
    whole(7, pbuf.at[0])
    to_head_groups(1, w_key)
    scoped("arrive", arrive, 0, 2, 0, 1)
    next_tables(3)
    for grp in range(GROUPS):
        for j in range(CORES):
            for q in range(seqs):
                ring_copy(0, 1, grp, j, q).wait_send()
    whole(8, sbuf)
    whole(9, sbuf)
    to_head_groups(2, w_value)
    prefetch()
    scoped("arrive", arrive, 0, 2, 1, 1)
    next_tables(4)
    for grp in range(GROUPS):
        send_first(1, grp, (1, 0))
    whole(10, pbuf.at[1])
    whole(11, pbuf.at[1])
    scoped("final", arrive, 0, 3, 0, 0)
    scoped("final", arrive, 0, 3, 1, 0)
    whole(12, pbuf.at[0])
    whole(13, pbuf.at[0])
    scoped("arrive", arrive, 1, 1, 0, 1)
    scoped("begin", begin_attention, 0)
    attend(1, 3)
    scoped("arrive", arrive, 1, 1, 1, 1)
    whole(14, pbuf.at[1])
    whole(15, pbuf.at[1])
    attend(3, 5)
    scoped("arrive", arrive, 1, 2, 0, 0)
    attend(5, 8)
    scoped("end", end_attention, 0)
    prefetch()
    scoped("arrive", arrive, 1, 2, 1, 0)
    scoped("final", arrive, 1, 3, 0, 1)
    scoped("final", arrive, 1, 3, 1, 1)
    scoped("begin", begin_attention, 1)
    attend(1, 8)
    scoped("end", end_attention, 1)
    scoped("out", out_copy(1).wait)

    for m in range(micros):
        for s, b in peers:
            key_copy(m, s, b).wait_send()
    for m, s in units:
        for j in range(CORES):
            table_copy(m, s, j).wait_send()
    for m in range(micros):
        for grp in range(GROUPS):
            for q in range(seqs):
                for s in range(1, chips):
                    for j in range(CORES):
                        if (m, s) != (0, 1):
                            ring_copy(m, s, grp, j, q).wait_send()
                rx_copy(m, grp, q).wait_send()
                if m == micros - 1:
                    y_copy(m, grp, q).wait_send()


def solution(mesh):
    stages = mesh.shape["pp"]
    ep_size = mesh.shape["ep"]
    tok_spec = P("pp", "data", "ep", None, None)
    vec_spec = P("pp", None)
    mat_spec = P("pp", None, None)
    head_spec = P("pp", None, None, None)

    def device_step(expert_out, expert_ids, slot_ids, gate_weights, residual, norm_moe, w_gate, w_up, w_down, norm_attn, w_query, w_key, w_value, w_out):
        micros, experts, slots_total, dim = expert_out.shape[1:]
        heads, head_dim = w_query.shape[2:]
        cap = slots_total // ep_size
        chips = ep_size // CORES
        half = dim // CORES
        seqs, seq_len, top_k = expert_ids.shape[2:]
        tok = seqs * seq_len
        group = tok // GROUPS
        width = 2 * head_dim
        head_groups = heads * head_dim // width

        def by_lane(x):
            return jnp.swapaxes(x[0], -1, -2)

        vmem = pl.BlockSpec(memory_space=pltpu.VMEM)
        anyspace = pl.BlockSpec(memory_space=pl.ANY)
        dma = pltpu.SemaphoreType.DMA
        out, _ = pl.pallas_call(
            functools.partial(boundary_kernel, stages, ep_size, seq_len),
            out_shape=[
                jax.ShapeDtypeStruct((micros, tok, dim), BF16),
                jax.ShapeDtypeStruct((3, head_groups, dim, width), BF16),
            ],
            in_specs=[anyspace, vmem, vmem, vmem, vmem, vmem, anyspace, anyspace, anyspace, vmem, anyspace, anyspace, anyspace, anyspace],
            out_specs=[anyspace, anyspace],
            scratch_shapes=[
                pltpu.VMEM((chips, CORES, experts, cap, half), BF16),
                pltpu.VMEM((2, CORES, experts, cap, half), BF16),
                pltpu.VMEM((2, 2, PARTS, tok, experts * cap), BF16),
                pltpu.VMEM((GROUPS, CORES, group, half), F32),
                pltpu.VMEM((2, GROUPS, CORES, group, half), F32),
                pltpu.VMEM((micros, chips - 1, GROUPS, CORES, group, half), F32),
                pltpu.VMEM((micros, GROUPS, group, half), F32),
                pltpu.VMEM((GROUPS, group, dim), BF16),
                pltpu.VMEM((micros, tok, dim), BF16),
                pltpu.VMEM((micros * tok, dim), BF16),
                pltpu.VMEM((2, 3, dim, width), BF16),
                pltpu.VMEM((2, width, dim), BF16),
                pltpu.VMEM((4, 128, heads, head_dim), BF16),
                pltpu.VMEM((4, head_groups, 128, width), BF16),
                pltpu.VMEM((tok, dim), BF16),
                pltpu.VMEM((tok, dim), F32),
                pltpu.VMEM((2, 3, tok, width), BF16),
                pltpu.VMEM((2, tok, width), BF16),
                pltpu.VMEM((micros, GROUPS, 2, top_k, group), F32),
                pltpu.VMEM((micros, GROUPS, chips * CORES, 2, top_k, group), F32),
                pltpu.VMEM((micros, GROUPS, group, chips * CORES * 2 * top_k), F32),
                dma((micros, chips, CORES)), dma((micros, chips, CORES)), dma((2, CORES)),
                dma((micros, chips - 1, GROUPS, CORES, seqs // GROUPS)), dma((micros, chips - 1, GROUPS, CORES, seqs // GROUPS)),
                dma((micros, GROUPS, seqs // GROUPS)), dma((micros, GROUPS, seqs // GROUPS)),
                dma((micros, GROUPS, seqs // GROUPS)), dma((micros, GROUPS, seqs // GROUPS)),
                dma((micros, chips, CORES)), dma((micros, chips, CORES)), dma((2, 4)), dma((4,)), dma((4,)), dma((micros,)),
                pltpu.SemaphoreType.REGULAR((chips,)),
            ],
            compiler_params=pltpu.CompilerParams(collective_id=0, has_side_effects=True, vmem_limit_bytes=67_000_000),
            cost_estimate=pl.CostEstimate(flops=50_000_000_000, bytes_accessed=200_000_000, transcendentals=0),
        )(expert_out[0], by_lane(expert_ids), by_lane(slot_ids), by_lane(gate_weights), residual[0].reshape(micros * tok, dim),
          norm_moe, w_gate[0], w_up[0], w_down[0], norm_attn, w_query[0], w_key[0], w_value[0], w_out[0].reshape(heads * head_dim, dim))
        return out.reshape(1, micros, seqs, seq_len, dim)

    in_specs = (tok_spec,) * 5 + (vec_spec, mat_spec, mat_spec, mat_spec, vec_spec, head_spec, head_spec, head_spec, head_spec)
    return jax.shard_map(device_step, mesh=mesh, in_specs=in_specs, out_specs=tok_spec, check_vma=False)
```

```python
import functools
import math
import jax
import jax.numpy as jnp
from jax import lax
from jax.experimental import pallas as pl
from jax.experimental.pallas import tpu as pltpu
from jax.sharding import PartitionSpec as P

EPSILON = 1e-6
CORES = 2
PARTS = 3
GROUPS = 2
MESH = pl.DeviceIdType.MESH
BF16_MAX = 3.3895313892515355e38
F32 = jnp.float32
BF16 = jnp.bfloat16


def dot(a, b):
    return jnp.dot(a, b, preferred_element_type=F32)


def boundary_kernel(stages, ep_size, seq_len,
                    eo, ids, slots, gates, resid_hbm, norm_moe, w_gate, w_up, w_down, norm_attn, w_query, w_key, w_value, w_out,
                    out, w_heads,
                    t_in, t_own, w, sbuf, pbuf, rbuf, rx, ysend, y_in, resid, shared, pool_in, pool_out, raw, turned, xn, acc, qkv, mixed, kp, kr, kt,
                    tab_send, tab_recv, own_sem, ring_send, ring_recv, rx_send, rx_recv, y_send, y_recv,
                    key_send, key_recv, load_sem, raw_sem, turn_sem, out_sem, resid_sem, free_sem):
    micros, experts, slots_total, dim = eo.shape
    chips = ep_size // CORES
    cap = slots_total // ep_size
    half = dim // CORES
    top_k = ids.shape[2]
    group = rbuf.shape[4]
    tok = group * GROUPS
    seqs = group // seq_len
    rows = experts * cap
    heads, head_dim = w_query.shape[1:]
    head_groups, width = w_heads.shape[1], w_heads.shape[3]
    ff = w_gate.shape[1]

    me = lax.axis_index("ep")
    pp = lax.axis_index("pp")
    chip, core = me // CORES, me % CORES
    other = 1 - core
    partner = chip * CORES + other
    step_mine = 1 + core * (chips - 2)
    step_other = 1 + other * (chips - 2)
    nxt = ((chip + step_mine) % chips) * CORES + core
    up = (pp + 1) % stages
    down = (pp + stages - 1) % stages

    peers = [(s, b) for s in range(1, chips + 1) for b in range(CORES) if (s, b) != (chips, 0)]

    def peer_id(s, b):
        there = (core + b) % CORES
        return ((chip + s * (1 + there * (chips - 2))) % chips) * CORES + there

    barrier = pltpu.get_barrier_semaphore()
    for s, b in peers:
        pl.semaphore_signal(barrier, inc=1, device_id={"ep": peer_id(s, b)}, device_id_type=MESH)
    pl.semaphore_signal(barrier, inc=1, device_id={"pp": down}, device_id_type=MESH)

    def dest_chip(s, stride):
        return (chip + (chips - s) * stride) % chips

    def cols(which):
        return pl.ds(pl.multiple_of(which * half, 128), half)

    def table_copy(m, s, j):
        dest = dest_chip(s, step_other) * CORES + (other + j) % CORES
        return pltpu.make_async_remote_copy(
            src_ref=eo.at[m, :, pl.ds(pl.multiple_of(dest * cap, 16), cap), cols(other)],
            dst_ref=t_in.at[s - 1, j], send_sem=tab_send.at[m, s - 1, j], recv_sem=tab_recv.at[m, s - 1, j],
            device_id={"ep": partner}, device_id_type=MESH)

    units = [(m, s) for m in range(micros) for s in range(1, chips + 1)]

    def own_copy(u, j):
        m, s = units[u]
        dest = dest_chip(s, step_mine) * CORES + (core + j) % CORES
        return pltpu.make_async_copy(
            eo.at[m, :, pl.ds(pl.multiple_of(dest * cap, 16), cap), cols(core)],
            t_own.at[u % 2, j], own_sem.at[u % 2, j])

    def load_own(u):
        for j in range(CORES):
            own_copy(u, j).start()

    load_own(0)
    load_own(1)
    resid_copy = pltpu.make_async_copy(resid_hbm, resid, resid_sem.at[0])
    resid_copy.start()

    def shared_loads():
        halves = [pl.ds(0, width), pl.ds(width, width)]
        return [
            pltpu.make_async_copy(w_gate.at[:, halves[0]], pool_in.at[0, 0], load_sem.at[0, 0]),
            pltpu.make_async_copy(w_gate.at[:, halves[1]], pool_in.at[0, 1], load_sem.at[0, 1]),
            pltpu.make_async_copy(w_up.at[:, halves[0]], pool_in.at[0, 2], load_sem.at[0, 2]),
            pltpu.make_async_copy(w_up.at[:, halves[1]], pool_in.at[1, 0], load_sem.at[1, 0]),
            pltpu.make_async_copy(w_down.at[halves[0]], pool_out.at[0], load_sem.at[0, 3]),
            pltpu.make_async_copy(w_down.at[halves[1]], pool_out.at[1], load_sem.at[1, 3]),
        ]

    first = me * cap
    for m in range(micros):
        for grp in range(GROUPS):
            packed, gate_rows = [], []
            for q in range(seqs):
                slot_here = slots[m, grp * seqs + q]
                key_here = ids[m, grp * seqs + q] * cap + (slot_here - first)
                packed.append(jnp.where(slot_here >= 0, key_here, -1).astype(F32))
                gate_rows.append(gates[m, grp * seqs + q])
            packed = jnp.concatenate(packed, axis=1)
            gate_rows = jnp.concatenate(gate_rows, axis=1)
            kp[m, grp, 0] = packed
            kp[m, grp, 1] = gate_rows
            kr[m, grp, (chips - 1) * CORES, 0] = packed
            kr[m, grp, (chips - 1) * CORES, 1] = gate_rows

    with jax.named_scope("barrier"):
        pl.semaphore_wait(barrier, len(peers) + 1)

    def key_copy(m, s, b):
        place = (s - 1) * CORES + b
        return pltpu.make_async_remote_copy(
            src_ref=kp.at[m], dst_ref=kr.at[m, :, place], send_sem=key_send.at[m, s - 1, b], recv_sem=key_recv.at[m, s - 1, b],
            device_id={"ep": peer_id(s, b)}, device_id_type=MESH)

    for m in range(micros):
        for s, b in peers:
            key_copy(m, s, b).start()
    for s in range(1, chips + 1):
        for j in range(CORES):
            table_copy(0, s, j).start()
    for copy in shared_loads():
        copy.start()

    key_rows = CORES * 2 * top_k

    def take_keys(m, s):
        for b in range(CORES):
            if (s, b) in peers:
                key_copy(m, s, b).wait_recv()
        for grp in range(GROUPS):
            arrived = kr[m, grp, (s - 1) * CORES:s * CORES].reshape(key_rows, group)
            kt[m, grp, :, (s - 1) * key_rows:s * key_rows] = arrived.T

    block = 32
    lane = lax.broadcasted_iota(jnp.int32, (block, rows), 1).astype(F32)

    def build_rows(v, grp, r0):
        m, s = units[v // CORES]
        base = ((s - 1) * CORES + v % CORES) * 2 * top_k
        known = kt[m, grp, pl.ds(r0, block), :]
        keys, scale = known[:, base:base + top_k], known[:, base + top_k:base + 2 * top_k]
        r1 = pl.multiple_of(grp * group + r0, block)
        for h, holder in enumerate((me, partner)):
            local = keys - (holder * rows).astype(F32)
            weights = jnp.zeros((block, rows), F32)
            for choice in range(top_k):
                weights = jnp.where(local[:, choice:choice + 1] == lane, scale[:, choice:choice + 1], weights)
            high = jnp.minimum(weights, BF16_MAX).astype(BF16)
            rest = weights - high.astype(F32)
            mid = rest.astype(BF16)
            low = (rest - mid.astype(F32)).astype(BF16)
            for part, value in enumerate((high, mid, low)):
                w[v % 2, h, part, pl.ds(r1, block), :] = value

    pieces = half // width
    subs = len(units) * CORES

    def step(v, target, groups, following):
        u, j = v // CORES, v % CORES
        m, s = units[u]
        if groups[0] == 0:
            own_copy(u, j).wait()
            table_copy(m, s, j).wait_recv()
        r0, count = groups[0] * group, len(groups) * group
        builds = [(w_next, grp, b) for w_next, grp in following for b in range(group // block)]
        per = -(-len(builds) // pieces)

        def body(n, _):
            c0 = pl.multiple_of(n * width, width)
            total = None
            for h in range(2):
                table = (t_own.at[u % 2, j] if h == 0 else t_in.at[s - 1, j])[:, :, pl.ds(c0, width)].reshape(rows, width)
                for part in range(PARTS):
                    term = dot(w[v % 2, h, part, r0:r0 + count], table)
                    total = term if total is None else total + term
            for i, grp in enumerate(groups):
                target[grp, j, :, pl.ds(c0, width)] = total[i * group:(i + 1) * group]
            for b in range(per):
                row = (n * per + b) * block
                if len(following) == 1:
                    build_rows(following[0][0], following[0][1], pl.multiple_of(row, block))
                elif following:
                    build_rows(following[0][0], row // group, pl.multiple_of(row % group, block))
            return 0

        lax.fori_loop(0, pieces, body, 0)
        if j == CORES - 1 and groups[-1] == GROUPS - 1:
            if u + 2 < len(units):
                load_own(u + 2)
            if m == 0:
                pl.semaphore_signal(free_sem.at[s - 1], inc=1, device_id={"ep": partner}, device_id_type=MESH)

    def whole(v, target):
        both = tuple(range(GROUPS))
        with jax.named_scope("step"):
            step(v, target, both, [(v + 1, grp) for grp in both] if v + 1 < subs else [])

    def next_tables(s):
        pl.semaphore_wait(free_sem.at[s - 1], 1)
        for j in range(CORES):
            table_copy(1, s, j).start()

    def ring_copy(m, s, grp, j, q):
        part = pl.ds(q * seq_len, seq_len)
        src = sbuf.at[grp, j, part] if s == 1 else rbuf.at[m, s - 2, grp, j, part]
        return pltpu.make_async_remote_copy(
            src_ref=src, dst_ref=rbuf.at[m, s - 1, grp, j, part],
            send_sem=ring_send.at[m, s - 1, grp, j, q], recv_sem=ring_recv.at[m, s - 1, grp, j, q],
            device_id={"ep": nxt}, device_id_type=MESH)

    def send_first(m, grp, order):
        for j in order:
            for q in range(seqs):
                ring_copy(m, 1, grp, j, q).start()

    def add_in(m, s, grp, j, q, slot):
        for b in range(seq_len // block):
            part = pl.ds(q * seq_len + b * block, block)
            rbuf[m, s - 1, grp, j, part, :] += pbuf[slot, grp, j, part, :]

    def rx_copy(m, grp, q):
        part = pl.ds(q * seq_len, seq_len)
        return pltpu.make_async_remote_copy(
            src_ref=rbuf.at[m, chips - 2, grp, 1, part], dst_ref=rx.at[m, grp, part],
            send_sem=rx_send.at[m, grp, q], recv_sem=rx_recv.at[m, grp, q],
            device_id={"ep": partner}, device_id_type=MESH)

    def arrive(m, s, grp, slot, which=None):
        for q in range(seqs) if which is None else which:
            for j in (1, 0):
                ring_copy(m, s, grp, j, q).wait_recv()
                add_in(m, s, grp, j, q, slot)
                if s < chips - 1:
                    ring_copy(m, s + 1, grp, j, q).start()
                elif j == 1:
                    rx_copy(m, grp, q).start()
            if s == chips - 1:
                combine(m, grp, q)

    def y_copy(m, grp, q):
        part = pl.ds(q * seq_len, seq_len)
        return pltpu.make_async_remote_copy(
            src_ref=ysend.at[grp, part], dst_ref=y_in.at[m, pl.ds(grp * group + q * seq_len, seq_len)],
            send_sem=y_send.at[m, grp, q], recv_sem=y_recv.at[m, grp, q],
            device_id={"pp": up}, device_id_type=MESH)

    def combine(m, grp, q):
        if m > 0:
            y_copy(m - 1, grp, q).wait_send()
        rx_copy(m, grp, q).wait_recv()

        def body(b, _):
            r0 = pl.multiple_of(q * seq_len + b * 16, 16)
            r1 = pl.multiple_of(m * tok + grp * group + r0, 16)
            for which, sums in ((core, rbuf.at[m, chips - 2, grp, 0]), (other, rx.at[m, grp])):
                base = resid[pl.ds(r1, 16), cols(which)].astype(F32) + shared[pl.ds(r1, 16), cols(which)].astype(F32)
                ysend[grp, pl.ds(r0, 16), cols(which)] = (base + sums[pl.ds(r0, 16), :]).astype(BF16)
            return 0

        lax.fori_loop(0, seq_len // 16, body, 0)
        y_copy(m, grp, q).start()

    def normalize(source, base, place, count, gain):
        def body(b, _):
            r0 = b * 16
            values = source[pl.ds(pl.multiple_of(base + r0, 16), 16), :].astype(F32)
            inv_rms = lax.rsqrt(jnp.mean(values * values, axis=-1, keepdims=True) + EPSILON)
            xn[pl.ds(pl.multiple_of(place + r0, 16), 16), :] = (values * inv_rms * gain[...]).astype(BF16)
            return 0
        lax.fori_loop(0, count // 16, body, 0, unroll=2)

    def shared_expert():
        for copy in shared_loads():
            copy.wait()
        resid_copy.wait()
        gate_refs = (pool_in.at[0, 0], pool_in.at[0, 1])
        up_refs = (pool_in.at[0, 2], pool_in.at[1, 0])

        def body(m, _):
            normalize(resid, m * tok, 0, tok, norm_moe)
            hidden = []
            for f in range(ff // width):
                gate_act = dot(xn[...], gate_refs[f][...])
                up_act = dot(xn[...], up_refs[f][...])
                hidden.append((gate_act * jax.nn.sigmoid(gate_act) * up_act).astype(BF16))
            r0 = pl.multiple_of(m * tok, 16)
            for n in range(dim // (2 * width)):
                span = pl.ds(n * 2 * width, 2 * width)
                total = dot(hidden[0], pool_out[0, :, span]) + dot(hidden[1], pool_out[1, :, span])
                shared[pl.ds(r0, tok), span] = total.astype(BF16)
            return 0

        lax.fori_loop(0, micros, body, 0)

    depth, chunk = raw.shape[:2]

    def to_head_groups(kind, source):
        count = dim // chunk

        def fetch(c):
            return pltpu.make_async_copy(source.at[pl.ds(pl.multiple_of(c * chunk, chunk), chunk)], raw.at[c % depth], raw_sem.at[c % depth])

        def flush(c):
            return pltpu.make_async_copy(turned.at[c % depth], w_heads.at[kind, :, pl.ds(pl.multiple_of(c * chunk, chunk), chunk)], turn_sem.at[c % depth])

        for c in range(depth - 1):
            fetch(c).start()

        def body(c, _):
            @pl.when(c + depth - 1 < count)
            def _():
                fetch(c + depth - 1).start()
            fetch(c).wait()

            @pl.when(c >= depth)
            def _():
                flush(c - depth).wait()

            def turn(b, _):
                r0 = pl.multiple_of(b * 32, 32)
                value = jnp.swapaxes(raw[c % depth, pl.ds(r0, 32)], 0, 1)
                for h in range(heads):
                    place = (h * head_dim) % width
                    turned[c % depth, h * head_dim // width, pl.ds(r0, 32), place:place + head_dim] = value[h]
                return 0

            lax.fori_loop(0, chunk // 32, turn, 0)
            flush(c).start()
            return 0

        with jax.named_scope("rewrite"):
            lax.fori_loop(0, count, body, 0)
            for c in range(count - depth, count):
                flush(c).wait()

    def in_loads(g, slot):
        return [pltpu.make_async_copy(w_heads.at[kind, g], pool_in.at[slot, kind], load_sem.at[slot, kind]) for kind in range(3)]

    def out_load(g, slot):
        return pltpu.make_async_copy(w_out.at[pl.ds(pl.multiple_of(g * width, width), width)], pool_out.at[slot], load_sem.at[slot, 3])

    ways = pool_out.shape[0]

    def prefetch():
        for g in range(ways):
            for copy in in_loads(g, g):
                copy.start()
            out_load(g, g).start()

    span_q = 128
    score_scale = 1.0 / math.sqrt(head_dim)

    spans = [(slice(r * span_q, (r + 1) * span_q), slice(h * head_dim, (h + 1) * head_dim))
             for r in range(tok // span_q) for h in range(width // head_dim)]

    def project(g, slot, kind):
        qkv[slot, kind] = dot(xn[...], pool_in[g % ways, kind]).astype(BF16)

    def score(slot):
        row = lax.broadcasted_iota(jnp.int32, (span_q, span_q), 0)
        col = lax.broadcasted_iota(jnp.int32, (span_q, span_q), 1)
        visible = (row >= col) & (row // seq_len == col // seq_len)
        scores = []
        for span in spans:
            product = lax.dot_general(qkv[(slot, 0) + span], qkv[(slot, 1) + span], (((1,), (1,)), ((), ())), preferred_element_type=F32)
            scores.append(jnp.where(visible, product * score_scale, -1e30))
        return scores

    def weigh(slot, scores):
        weighed = []
        for values in scores:
            probs = jnp.exp(values - jnp.max(values, axis=-1, keepdims=True))
            weighed.append((probs.astype(BF16), jnp.sum(probs, axis=-1, keepdims=True)))
        for span, (probs, total) in zip(spans, weighed):
            mixed[(slot,) + span] = (dot(probs, qkv[(slot, 2) + span]) / total).astype(BF16)

    def project_out(g, slot):
        for n in range(dim // (2 * width)):
            span = pl.ds(n * 2 * width, 2 * width)
            acc[:, span] += dot(mixed[slot], pool_out[g % ways, :, span])

    def advance(g, slot):
        for copy in in_loads(g, g % ways):
            copy.wait()
        out_load(g - 1, (g - 1) % ways).wait()
        project(g, slot, 0)
        scores = score(1 - slot)
        project(g, slot, 1)
        weigh(1 - slot, scores)
        project(g, slot, 2)
        project_out(g - 1, 1 - slot)

        @pl.when(g + ways < head_groups)
        def _():
            for copy in in_loads(g + ways, g % ways):
                copy.start()

        @pl.when(g - 1 + ways < head_groups)
        def _():
            out_load(g - 1 + ways, (g - 1) % ways).start()

    def attend(g0, pairs):
        def body(i, _):
            advance(g0 + 2 * i, g0 % 2)
            advance(g0 + 2 * i + 1, 1 - g0 % 2)
            return 0

        with jax.named_scope("attend"):
            lax.fori_loop(0, pairs, body, 0)

    def out_copy(m):
        return pltpu.make_async_copy(xn, out.at[m], out_sem.at[m])

    def take_y(m, grp, q):
        y_copy(m, grp, q).wait_recv()
        start = grp * group + q * seq_len
        normalize(y_in.at[m], start, start, seq_len, norm_attn)

    def clear_sums():
        def clear(b, _):
            acc[pl.ds(pl.multiple_of(b * 16, 16), 16), :] = jnp.zeros((16, dim), F32)
            return 0

        lax.fori_loop(0, tok // 16, clear, 0)

    def begin_attention():
        for copy in in_loads(0, 0):
            copy.wait()
        for kind in range(3):
            project(0, 0, kind)
        for copy in in_loads(ways, 0):
            copy.start()

    def end_attention(m):
        advance(head_groups - 1, 1)
        out_load(head_groups - 1, (head_groups - 1) % ways).wait()
        weigh(1, score(1))
        project_out(head_groups - 1, 1)

        def body(b, _):
            r0 = pl.multiple_of(b * 16, 16)
            proj = acc[pl.ds(r0, 16), :].astype(BF16).astype(F32)
            xn[pl.ds(r0, 16), :] = (y_in[m, pl.ds(r0, 16), :].astype(F32) + proj).astype(BF16)
            return 0

        lax.fori_loop(0, tok // 16, body, 0)
        out_copy(m).start()

    def scoped(name, task, *args):
        with jax.named_scope(name):
            task(*args)

    def first_rows(b, _):
        build_rows(0, 0, pl.multiple_of(b * block, block))
        return 0

    scoped("keys", take_keys, 0, 1)
    scoped("build", lax.fori_loop, 0, group // block, first_rows, 0)
    for grp in range(GROUPS):
        for j in range(CORES):
            if (grp, j) == (1, 1):
                following = [(2, 0), (2, 1)]
            else:
                following = [((j + 1) % CORES, grp + j)]
            scoped("half", step, j, sbuf, (grp,), following)
            send_first(0, grp, (j,))
            if (grp, j) == (0, 1):
                for m, s in units[1:]:
                    scoped("keys", take_keys, m, s)
    whole(2, pbuf.at[0])
    whole(3, pbuf.at[0])
    scoped("shared", shared_expert)
    scoped("arrive", arrive, 0, 1, 0, 0)
    next_tables(1)
    to_head_groups(0, w_query)
    whole(4, pbuf.at[1])
    whole(5, pbuf.at[1])
    scoped("arrive", arrive, 0, 1, 1, 0)
    next_tables(2)
    whole(6, pbuf.at[0])
    whole(7, pbuf.at[0])
    scoped("arrive", arrive, 0, 2, 0, 1)
    next_tables(3)
    for grp in range(GROUPS):
        for j in range(CORES):
            for q in range(seqs):
                ring_copy(0, 1, grp, j, q).wait_send()
    whole(8, sbuf)
    whole(9, sbuf)
    to_head_groups(1, w_key)
    scoped("arrive", arrive, 0, 2, 1, 1)
    next_tables(4)
    for grp in range(GROUPS):
        send_first(1, grp, (1, 0))
    whole(10, pbuf.at[1])
    whole(11, pbuf.at[1])
    scoped("final", arrive, 0, 3, 0, 0)
    to_head_groups(2, w_value)
    prefetch()
    scoped("final", arrive, 0, 3, 1, 0)
    whole(12, pbuf.at[0])
    whole(13, pbuf.at[0])
    scoped("arrive", arrive, 1, 1, 0, 1)
    clear_sums()
    for grp in range(GROUPS):
        for q in range(seqs):
            scoped("take_y", take_y, 0, grp, q)
    scoped("begin", begin_attention)
    attend(1, 3)
    scoped("arrive", arrive, 1, 1, 1, 1)
    whole(14, pbuf.at[1])
    whole(15, pbuf.at[1])
    scoped("end", end_attention, 0)
    prefetch()
    scoped("arrive", arrive, 1, 2, 0, 0)
    scoped("arrive", arrive, 1, 2, 1, 0)
    out_copy(0).wait()
    clear_sums()
    scoped("final", arrive, 1, 3, 0, 1)
    scoped("take_y", take_y, 1, 0, 0)
    scoped("final", arrive, 1, 3, 1, 1, (0,))
    scoped("take_y", take_y, 1, 0, 1)
    scoped("final", arrive, 1, 3, 1, 1, (1,))
    scoped("take_y", take_y, 1, 1, 0)
    scoped("take_y", take_y, 1, 1, 1)
    scoped("begin", begin_attention)
    attend(1, 3)
    scoped("end", end_attention, 1)
    scoped("out", out_copy(1).wait)

    for m in range(micros):
        for s, b in peers:
            key_copy(m, s, b).wait_send()
    for m, s in units:
        for j in range(CORES):
            table_copy(m, s, j).wait_send()
    for m in range(micros):
        for grp in range(GROUPS):
            for q in range(seqs):
                for s in range(1, chips):
                    for j in range(CORES):
                        if (m, s) != (0, 1):
                            ring_copy(m, s, grp, j, q).wait_send()
                rx_copy(m, grp, q).wait_send()
                if m == micros - 1:
                    y_copy(m, grp, q).wait_send()


def solution(mesh):
    stages = mesh.shape["pp"]
    ep_size = mesh.shape["ep"]
    tok_spec = P("pp", "data", "ep", None, None)
    vec_spec = P("pp", None)
    mat_spec = P("pp", None, None)
    head_spec = P("pp", None, None, None)

    def device_step(expert_out, expert_ids, slot_ids, gate_weights, residual, norm_moe, w_gate, w_up, w_down, norm_attn, w_query, w_key, w_value, w_out):
        micros, experts, slots_total, dim = expert_out.shape[1:]
        heads, head_dim = w_query.shape[2:]
        cap = slots_total // ep_size
        chips = ep_size // CORES
        half = dim // CORES
        seqs, seq_len, top_k = expert_ids.shape[2:]
        tok = seqs * seq_len
        group = tok // GROUPS
        width = 2 * head_dim
        head_groups = heads * head_dim // width

        def by_lane(x):
            return jnp.swapaxes(x[0], -1, -2)

        vmem = pl.BlockSpec(memory_space=pltpu.VMEM)
        anyspace = pl.BlockSpec(memory_space=pl.ANY)
        dma = pltpu.SemaphoreType.DMA
        out, _ = pl.pallas_call(
            functools.partial(boundary_kernel, stages, ep_size, seq_len),
            out_shape=[
                jax.ShapeDtypeStruct((micros, tok, dim), BF16),
                jax.ShapeDtypeStruct((3, head_groups, dim, width), BF16),
            ],
            in_specs=[anyspace, vmem, vmem, vmem, anyspace, vmem, anyspace, anyspace, anyspace, vmem, anyspace, anyspace, anyspace, anyspace],
            out_specs=[anyspace, anyspace],
            scratch_shapes=[
                pltpu.VMEM((chips, CORES, experts, cap, half), BF16),
                pltpu.VMEM((2, CORES, experts, cap, half), BF16),
                pltpu.VMEM((2, 2, PARTS, tok, experts * cap), BF16),
                pltpu.VMEM((GROUPS, CORES, group, half), F32),
                pltpu.VMEM((2, GROUPS, CORES, group, half), F32),
                pltpu.VMEM((micros, chips - 1, GROUPS, CORES, group, half), F32),
                pltpu.VMEM((micros, GROUPS, group, half), F32),
                pltpu.VMEM((GROUPS, group, dim), BF16),
                pltpu.VMEM((micros, tok, dim), BF16),
                pltpu.VMEM((micros * tok, dim), BF16),
                pltpu.VMEM((micros * tok, dim), BF16),
                pltpu.VMEM((3, 3, dim, width), BF16),
                pltpu.VMEM((3, width, dim), BF16),
                pltpu.VMEM((3, 128, heads, head_dim), BF16),
                pltpu.VMEM((3, head_groups, 128, width), BF16),
                pltpu.VMEM((tok, dim), BF16),
                pltpu.VMEM((tok, dim), F32),
                pltpu.VMEM((2, 3, tok, width), BF16),
                pltpu.VMEM((2, tok, width), BF16),
                pltpu.VMEM((micros, GROUPS, 2, top_k, group), F32),
                pltpu.VMEM((micros, GROUPS, chips * CORES, 2, top_k, group), F32),
                pltpu.VMEM((micros, GROUPS, group, chips * CORES * 2 * top_k), F32),
                dma((micros, chips, CORES)), dma((micros, chips, CORES)), dma((2, CORES)),
                dma((micros, chips - 1, GROUPS, CORES, seqs // GROUPS)), dma((micros, chips - 1, GROUPS, CORES, seqs // GROUPS)),
                dma((micros, GROUPS, seqs // GROUPS)), dma((micros, GROUPS, seqs // GROUPS)),
                dma((micros, GROUPS, seqs // GROUPS)), dma((micros, GROUPS, seqs // GROUPS)),
                dma((micros, chips, CORES)), dma((micros, chips, CORES)), dma((3, 4)), dma((3,)), dma((3,)), dma((micros,)), dma((1,)),
                pltpu.SemaphoreType.REGULAR((chips,)),
            ],
            compiler_params=pltpu.CompilerParams(collective_id=0, has_side_effects=True, vmem_limit_bytes=67_000_000),
            cost_estimate=pl.CostEstimate(flops=50_000_000_000, bytes_accessed=200_000_000, transcendentals=0),
        )(expert_out[0], by_lane(expert_ids), by_lane(slot_ids), by_lane(gate_weights), residual[0].reshape(micros * tok, dim),
          norm_moe, w_gate[0], w_up[0], w_down[0], norm_attn, w_query[0], w_key[0], w_value[0], w_out[0].reshape(heads * head_dim, dim))
        return out.reshape(1, micros, seqs, seq_len, dim)

    in_specs = (tok_spec,) * 5 + (vec_spec, mat_spec, mat_spec, mat_spec, vec_spec, head_spec, head_spec, head_spec, head_spec)
    return jax.shard_map(device_step, mesh=mesh, in_specs=in_specs, out_specs=tok_spec, check_vma=False)
```

```python
import functools
import math
import jax
import jax.numpy as jnp
from jax import lax
from jax.experimental import pallas as pl
from jax.experimental.pallas import tpu as pltpu
from jax.sharding import PartitionSpec as P

EPSILON = 1e-6
CORES = 2
PARTS = 3
GROUPS = 2
MESH = pl.DeviceIdType.MESH
BF16_MAX = 3.3895313892515355e38
F32 = jnp.float32
BF16 = jnp.bfloat16


def dot(a, b):
    return jnp.dot(a, b, preferred_element_type=F32)


def boundary_kernel(stages, ep_size, seq_len,
                    eo, ids, slots, gates, resid_hbm, norm_moe, w_gate, w_up, w_down, norm_attn, w_query, w_key, w_value, w_out,
                    out, w_heads,
                    t_in, t_own, w, sbuf, pbuf, rbuf, rx, ysend, y_in, resid, shared, pool_in, pool_out, raw, turned, xn, acc, qkv, mixed, kp, kr, kt,
                    tab_send, tab_recv, own_sem, ring_send, ring_recv, rx_send, rx_recv, y_send, y_recv,
                    key_send, key_recv, load_sem, raw_sem, turn_sem, out_sem, resid_sem, free_sem):
    micros, experts, slots_total, dim = eo.shape
    chips = ep_size // CORES
    cap = slots_total // ep_size
    half = dim // CORES
    top_k = ids.shape[2]
    group = rbuf.shape[4]
    tok = group * GROUPS
    seqs = group // seq_len
    rows = experts * cap
    heads, head_dim = w_query.shape[1:]
    head_groups, width = w_heads.shape[1], w_heads.shape[3]
    ff = w_gate.shape[1]

    me = lax.axis_index("ep")
    pp = lax.axis_index("pp")
    chip, core = me // CORES, me % CORES
    other = 1 - core
    partner = chip * CORES + other
    step_mine = 1 + core * (chips - 2)
    step_other = 1 + other * (chips - 2)
    nxt = ((chip + step_mine) % chips) * CORES + core
    up = (pp + 1) % stages
    down = (pp + stages - 1) % stages

    peers = [(s, b) for s in range(1, chips + 1) for b in range(CORES) if (s, b) != (chips, 0)]

    def peer_id(s, b):
        there = (core + b) % CORES
        return ((chip + s * (1 + there * (chips - 2))) % chips) * CORES + there

    barrier = pltpu.get_barrier_semaphore()
    for s, b in peers:
        pl.semaphore_signal(barrier, inc=1, device_id={"ep": peer_id(s, b)}, device_id_type=MESH)
    pl.semaphore_signal(barrier, inc=1, device_id={"pp": down}, device_id_type=MESH)

    def dest_chip(s, stride):
        return (chip + (chips - s) * stride) % chips

    def cols(which):
        return pl.ds(pl.multiple_of(which * half, 128), half)

    def table_copy(m, s, j):
        dest = dest_chip(s, step_other) * CORES + (other + j) % CORES
        return pltpu.make_async_remote_copy(
            src_ref=eo.at[m, :, pl.ds(pl.multiple_of(dest * cap, 16), cap), cols(other)],
            dst_ref=t_in.at[s - 1, j], send_sem=tab_send.at[m, s - 1, j], recv_sem=tab_recv.at[m, s - 1, j],
            device_id={"ep": partner}, device_id_type=MESH)

    units = [(m, s) for m in range(micros) for s in range(1, chips + 1)]

    def own_copy(u, j):
        m, s = units[u]
        dest = dest_chip(s, step_mine) * CORES + (core + j) % CORES
        return pltpu.make_async_copy(
            eo.at[m, :, pl.ds(pl.multiple_of(dest * cap, 16), cap), cols(core)],
            t_own.at[u % 2, j], own_sem.at[u % 2, j])

    def load_own(u):
        for j in range(CORES):
            own_copy(u, j).start()

    load_own(0)
    load_own(1)
    resid_copy = pltpu.make_async_copy(resid_hbm, resid, resid_sem.at[0])
    resid_copy.start()

    def shared_loads():
        halves = [pl.ds(0, width), pl.ds(width, width)]
        return [
            pltpu.make_async_copy(w_gate.at[:, halves[0]], pool_in.at[0, 0], load_sem.at[0, 0]),
            pltpu.make_async_copy(w_gate.at[:, halves[1]], pool_in.at[0, 1], load_sem.at[0, 1]),
            pltpu.make_async_copy(w_up.at[:, halves[0]], pool_in.at[0, 2], load_sem.at[0, 2]),
            pltpu.make_async_copy(w_up.at[:, halves[1]], pool_in.at[1, 0], load_sem.at[1, 0]),
            pltpu.make_async_copy(w_down.at[halves[0]], pool_out.at[0], load_sem.at[0, 3]),
            pltpu.make_async_copy(w_down.at[halves[1]], pool_out.at[1], load_sem.at[1, 3]),
        ]

    first = me * cap
    for m in range(micros):
        for grp in range(GROUPS):
            packed, gate_rows = [], []
            for q in range(seqs):
                slot_here = slots[m, grp * seqs + q]
                key_here = ids[m, grp * seqs + q] * cap + (slot_here - first)
                packed.append(jnp.where(slot_here >= 0, key_here, -1).astype(F32))
                gate_rows.append(gates[m, grp * seqs + q])
            packed = jnp.concatenate(packed, axis=1)
            gate_rows = jnp.concatenate(gate_rows, axis=1)
            kp[m, grp, 0] = packed
            kp[m, grp, 1] = gate_rows
            kr[m, grp, (chips - 1) * CORES, 0] = packed
            kr[m, grp, (chips - 1) * CORES, 1] = gate_rows

    with jax.named_scope("barrier"):
        pl.semaphore_wait(barrier, len(peers) + 1)

    def key_copy(m, s, b):
        place = (s - 1) * CORES + b
        return pltpu.make_async_remote_copy(
            src_ref=kp.at[m], dst_ref=kr.at[m, :, place], send_sem=key_send.at[m, s - 1, b], recv_sem=key_recv.at[m, s - 1, b],
            device_id={"ep": peer_id(s, b)}, device_id_type=MESH)

    for m in range(micros):
        for s, b in peers:
            key_copy(m, s, b).start()
    for s in range(1, chips + 1):
        for j in range(CORES):
            table_copy(0, s, j).start()
    for copy in shared_loads():
        copy.start()

    key_rows = CORES * 2 * top_k

    def take_keys(m, s):
        for b in range(CORES):
            if (s, b) in peers:
                key_copy(m, s, b).wait_recv()
        for grp in range(GROUPS):
            arrived = kr[m, grp, (s - 1) * CORES:s * CORES].reshape(key_rows, group)
            kt[m, grp, :, (s - 1) * key_rows:s * key_rows] = arrived.T

    block = 32
    lane = lax.broadcasted_iota(jnp.int32, (block, rows), 1).astype(F32)

    def build_rows(v, grp, r0):
        m, s = units[v // CORES]
        base = ((s - 1) * CORES + v % CORES) * 2 * top_k
        known = kt[m, grp, pl.ds(r0, block), :]
        keys, scale = known[:, base:base + top_k], known[:, base + top_k:base + 2 * top_k]
        r1 = pl.multiple_of(grp * group + r0, block)
        for h, holder in enumerate((me, partner)):
            local = keys - (holder * rows).astype(F32)
            weights = jnp.zeros((block, rows), F32)
            for choice in range(top_k):
                weights = jnp.where(local[:, choice:choice + 1] == lane, scale[:, choice:choice + 1], weights)
            high = jnp.minimum(weights, BF16_MAX).astype(BF16)
            rest = weights - high.astype(F32)
            mid = rest.astype(BF16)
            low = (rest - mid.astype(F32)).astype(BF16)
            for part, value in enumerate((high, mid, low)):
                w[v % 2, h, part, pl.ds(r1, block), :] = value

    pieces = half // width
    subs = len(units) * CORES

    def step(v, target, groups, following):
        u, j = v // CORES, v % CORES
        m, s = units[u]
        if groups[0] == 0:
            own_copy(u, j).wait()
            table_copy(m, s, j).wait_recv()
        r0, count = groups[0] * group, len(groups) * group
        builds = [(w_next, grp, b) for w_next, grp in following for b in range(group // block)]
        per = -(-len(builds) // pieces)

        def body(n, _):
            c0 = pl.multiple_of(n * width, width)
            total = None
            for h in range(2):
                table = (t_own.at[u % 2, j] if h == 0 else t_in.at[s - 1, j])[:, :, pl.ds(c0, width)].reshape(rows, width)
                for part in range(PARTS):
                    term = dot(w[v % 2, h, part, r0:r0 + count], table)
                    total = term if total is None else total + term
            for i, grp in enumerate(groups):
                target[grp, j, :, pl.ds(c0, width)] = total[i * group:(i + 1) * group]
            for b in range(per):
                row = (n * per + b) * block
                if len(following) == 1:
                    build_rows(following[0][0], following[0][1], pl.multiple_of(row, block))
                elif following:
                    build_rows(following[0][0], row // group, pl.multiple_of(row % group, block))
            return 0

        lax.fori_loop(0, pieces, body, 0)
        if j == CORES - 1 and groups[-1] == GROUPS - 1:
            if u + 2 < len(units):
                load_own(u + 2)
            if m == 0:
                pl.semaphore_signal(free_sem.at[s - 1], inc=1, device_id={"ep": partner}, device_id_type=MESH)

    def whole(v, target):
        both = tuple(range(GROUPS))
        with jax.named_scope("step"):
            step(v, target, both, [(v + 1, grp) for grp in both] if v + 1 < subs else [])

    def next_tables(s):
        pl.semaphore_wait(free_sem.at[s - 1], 1)
        for j in range(CORES):
            table_copy(1, s, j).start()

    def ring_copy(m, s, grp, j, q):
        part = pl.ds(q * seq_len, seq_len)
        src = sbuf.at[grp, j, part] if s == 1 else rbuf.at[m, s - 2, grp, j, part]
        return pltpu.make_async_remote_copy(
            src_ref=src, dst_ref=rbuf.at[m, s - 1, grp, j, part],
            send_sem=ring_send.at[m, s - 1, grp, j, q], recv_sem=ring_recv.at[m, s - 1, grp, j, q],
            device_id={"ep": nxt}, device_id_type=MESH)

    def send_first(m, grp, order):
        for j in order:
            for q in range(seqs):
                ring_copy(m, 1, grp, j, q).start()

    def add_in(m, s, grp, j, q, slot):
        for b in range(seq_len // block):
            part = pl.ds(q * seq_len + b * block, block)
            rbuf[m, s - 1, grp, j, part, :] += pbuf[slot, grp, j, part, :]

    def rx_copy(m, grp, q):
        part = pl.ds(q * seq_len, seq_len)
        return pltpu.make_async_remote_copy(
            src_ref=rbuf.at[m, chips - 2, grp, 1, part], dst_ref=rx.at[m, grp, part],
            send_sem=rx_send.at[m, grp, q], recv_sem=rx_recv.at[m, grp, q],
            device_id={"ep": partner}, device_id_type=MESH)

    def arrive(m, s, grp, slot, which=None):
        for q in range(seqs) if which is None else which:
            for j in (1, 0):
                ring_copy(m, s, grp, j, q).wait_recv()
                add_in(m, s, grp, j, q, slot)
                if s < chips - 1:
                    ring_copy(m, s + 1, grp, j, q).start()
                elif j == 1:
                    rx_copy(m, grp, q).start()
            if s == chips - 1:
                combine(m, grp, q)

    def y_copy(m, grp, q):
        part = pl.ds(q * seq_len, seq_len)
        return pltpu.make_async_remote_copy(
            src_ref=ysend.at[grp, part], dst_ref=y_in.at[m, pl.ds(grp * group + q * seq_len, seq_len)],
            send_sem=y_send.at[m, grp, q], recv_sem=y_recv.at[m, grp, q],
            device_id={"pp": up}, device_id_type=MESH)

    def combine(m, grp, q):
        if m > 0:
            y_copy(m - 1, grp, q).wait_send()
        rx_copy(m, grp, q).wait_recv()

        def body(b, _):
            r0 = pl.multiple_of(q * seq_len + b * 16, 16)
            r1 = pl.multiple_of(m * tok + grp * group + r0, 16)
            for which, sums in ((core, rbuf.at[m, chips - 2, grp, 0]), (other, rx.at[m, grp])):
                base = resid[pl.ds(r1, 16), cols(which)].astype(F32) + shared[pl.ds(r1, 16), cols(which)].astype(F32)
                ysend[grp, pl.ds(r0, 16), cols(which)] = (base + sums[pl.ds(r0, 16), :]).astype(BF16)
            return 0

        lax.fori_loop(0, seq_len // 16, body, 0)
        y_copy(m, grp, q).start()

    def normalize(source, base, place, count, gain):
        def body(b, _):
            r0 = b * 16
            values = source[pl.ds(pl.multiple_of(base + r0, 16), 16), :].astype(F32)
            inv_rms = lax.rsqrt(jnp.mean(values * values, axis=-1, keepdims=True) + EPSILON)
            xn[pl.ds(pl.multiple_of(place + r0, 16), 16), :] = (values * inv_rms * gain[...]).astype(BF16)
            return 0
        lax.fori_loop(0, count // 16, body, 0, unroll=2)

    def shared_expert():
        for copy in shared_loads():
            copy.wait()
        resid_copy.wait()
        gate_refs = (pool_in.at[0, 0], pool_in.at[0, 1])
        up_refs = (pool_in.at[0, 2], pool_in.at[1, 0])

        def body(m, _):
            normalize(resid, m * tok, 0, tok, norm_moe)
            hidden = []
            for f in range(ff // width):
                gate_act = dot(xn[...], gate_refs[f][...])
                up_act = dot(xn[...], up_refs[f][...])
                hidden.append((gate_act * jax.nn.sigmoid(gate_act) * up_act).astype(BF16))
            r0 = pl.multiple_of(m * tok, 16)
            for n in range(dim // (2 * width)):
                span = pl.ds(n * 2 * width, 2 * width)
                total = dot(hidden[0], pool_out[0, :, span]) + dot(hidden[1], pool_out[1, :, span])
                shared[pl.ds(r0, tok), span] = total.astype(BF16)
            return 0

        lax.fori_loop(0, micros, body, 0)

    depth, chunk = raw.shape[:2]

    def to_head_groups(kind, source):
        count = dim // chunk

        def fetch(c):
            return pltpu.make_async_copy(source.at[pl.ds(pl.multiple_of(c * chunk, chunk), chunk)], raw.at[c % depth], raw_sem.at[c % depth])

        def flush(c):
            return pltpu.make_async_copy(turned.at[c % depth], w_heads.at[kind, :, pl.ds(pl.multiple_of(c * chunk, chunk), chunk)], turn_sem.at[c % depth])

        for c in range(depth - 1):
            fetch(c).start()

        def body(c, _):
            @pl.when(c + depth - 1 < count)
            def _():
                fetch(c + depth - 1).start()
            fetch(c).wait()

            @pl.when(c >= depth)
            def _():
                flush(c - depth).wait()

            def turn(b, _):
                r0 = pl.multiple_of(b * 32, 32)
                value = jnp.swapaxes(raw[c % depth, pl.ds(r0, 32)], 0, 1)
                for h in range(heads):
                    place = (h * head_dim) % width
                    turned[c % depth, h * head_dim // width, pl.ds(r0, 32), place:place + head_dim] = value[h]
                return 0

            lax.fori_loop(0, chunk // 32, turn, 0)
            flush(c).start()
            return 0

        with jax.named_scope("rewrite"):
            lax.fori_loop(0, count, body, 0)
            for c in range(count - depth, count):
                flush(c).wait()

    def in_loads(g, slot):
        return [pltpu.make_async_copy(w_heads.at[kind, g], pool_in.at[slot, kind], load_sem.at[slot, kind]) for kind in range(3)]

    def out_load(g, slot):
        return pltpu.make_async_copy(w_out.at[pl.ds(pl.multiple_of(g * width, width), width)], pool_out.at[slot], load_sem.at[slot, 3])

    ways = pool_out.shape[0]

    def prefetch():
        for g in range(ways):
            for copy in in_loads(g, g):
                copy.start()
            out_load(g, g).start()

    span_q = 128
    score_scale = 1.0 / math.sqrt(head_dim)

    def bounds(grps):
        return grps[0] * group, len(grps) * group

    def spans(count):
        return [(slice(r * span_q, (r + 1) * span_q), slice(h * head_dim, (h + 1) * head_dim))
                for r in range(count // span_q) for h in range(width // head_dim)]

    def project(g, slot, kind, grps, shift):
        lo, count = bounds(grps)
        qkv[slot, kind, :count] = dot(xn[lo:lo + count], pool_in[(g + shift) % ways, kind]).astype(BF16)

    def score(slot, count):
        row = lax.broadcasted_iota(jnp.int32, (span_q, span_q), 0)
        col = lax.broadcasted_iota(jnp.int32, (span_q, span_q), 1)
        visible = (row >= col) & (row // seq_len == col // seq_len)
        scores = []
        for span in spans(count):
            product = lax.dot_general(qkv[(slot, 0) + span], qkv[(slot, 1) + span], (((1,), (1,)), ((), ())), preferred_element_type=F32)
            scores.append(jnp.where(visible, product * score_scale, -1e30))
        return scores

    def weigh(scores):
        weighed = []
        for values in scores:
            probs = jnp.exp(values - jnp.max(values, axis=-1, keepdims=True))
            weighed.append((probs.astype(BF16), jnp.sum(probs, axis=-1, keepdims=True)))
        return weighed

    def gather_values(slot, weighed, count):
        for span, (probs, total) in zip(spans(count), weighed):
            mixed[(slot,) + span] = (dot(probs, qkv[(slot, 2) + span]) / total).astype(BF16)

    def project_out(g, slot, grps, shift):
        lo, count = bounds(grps)
        for n in range(dim // (2 * width)):
            span = pl.ds(n * 2 * width, 2 * width)
            acc[lo:lo + count, span] += dot(mixed[slot, :count], pool_out[(g + shift) % ways, :, span])

    def advance(g, slot, grps, shift, again):
        lo, count = bounds(grps)
        last = 1 - slot
        for copy in in_loads(g, (g + shift) % ways):
            copy.wait()
        out_load(g - 1, (g - 1 + shift) % ways).wait()
        if count == span_q:
            scores = score(last, count)
            project(g, slot, 0, grps, shift)
            weighed = weigh(scores)
            project(g, slot, 1, grps, shift)
            gather_values(last, weighed, count)
        else:
            project(g, slot, 0, grps, shift)
            scores = score(last, count)
            project(g, slot, 1, grps, shift)
            gather_values(last, weigh(scores), count)
        project(g, slot, 2, grps, shift)
        project_out(g - 1, last, grps, shift)

        @pl.when(again | (g + ways < head_groups))
        def _():
            for copy in in_loads((g + ways) % head_groups, (g + shift) % ways):
                copy.start()

        @pl.when(again | (g - 1 + ways < head_groups))
        def _():
            out_load((g - 1 + ways) % head_groups, (g - 1 + shift) % ways).start()

    def attend(g0, pairs, grps, shift, again):
        def body(i, _):
            advance(g0 + 2 * i, g0 % 2, grps, shift, again)
            advance(g0 + 2 * i + 1, 1 - g0 % 2, grps, shift, again)
            return 0

        with jax.named_scope("attend"):
            lax.fori_loop(0, pairs, body, 0)

    def out_copy(m, grps):
        part = pl.ds(*bounds(grps))
        return pltpu.make_async_copy(xn.at[part], out.at[m, part], out_sem.at[m, grps[0]])

    def take_y(m, grp, q):
        y_copy(m, grp, q).wait_recv()
        start = grp * group + q * seq_len
        normalize(y_in.at[m], start, start, seq_len, norm_attn)

    def clear_sums():
        def clear(b, _):
            acc[pl.ds(pl.multiple_of(b * 16, 16), 16), :] = jnp.zeros((16, dim), F32)
            return 0

        lax.fori_loop(0, tok // 16, clear, 0)

    def begin_attention(grps, shift):
        for copy in in_loads(0, shift % ways):
            copy.wait()
        for kind in range(3):
            project(0, 0, kind, grps, shift)
        for copy in in_loads(ways, shift % ways):
            copy.start()

    def end_attention(m, grps, shift, again):
        lo, count = bounds(grps)
        final = head_groups - 1
        advance(final, 1, grps, shift, again)
        out_load(final, (final + shift) % ways).wait()
        gather_values(1, weigh(score(1, count)), count)
        project_out(final, 1, grps, shift)
        if again:
            out_load((final + ways) % head_groups, (final + shift) % ways).start()

        def body(b, _):
            r0 = pl.multiple_of(lo + b * 16, 16)
            proj = acc[pl.ds(r0, 16), :].astype(BF16).astype(F32)
            xn[pl.ds(r0, 16), :] = (y_in[m, pl.ds(r0, 16), :].astype(F32) + proj).astype(BF16)
            return 0

        lax.fori_loop(0, count // 16, body, 0)
        out_copy(m, grps).start()

    def scoped(name, task, *args):
        with jax.named_scope(name):
            task(*args)

    def first_rows(b, _):
        build_rows(0, 0, pl.multiple_of(b * block, block))
        return 0

    scoped("keys", take_keys, 0, 1)
    scoped("build", lax.fori_loop, 0, group // block, first_rows, 0)
    for grp in range(GROUPS):
        for j in range(CORES):
            if (grp, j) == (1, 1):
                following = [(2, 0), (2, 1)]
            else:
                following = [((j + 1) % CORES, grp + j)]
            scoped("half", step, j, sbuf, (grp,), following)
            send_first(0, grp, (j,))
            if (grp, j) == (0, 1):
                for m, s in units[1:]:
                    scoped("keys", take_keys, m, s)
    whole(2, pbuf.at[0])
    whole(3, pbuf.at[0])
    scoped("shared", shared_expert)
    scoped("arrive", arrive, 0, 1, 0, 0)
    next_tables(1)
    to_head_groups(0, w_query)
    whole(4, pbuf.at[1])
    whole(5, pbuf.at[1])
    scoped("arrive", arrive, 0, 1, 1, 0)
    next_tables(2)
    whole(6, pbuf.at[0])
    whole(7, pbuf.at[0])
    scoped("arrive", arrive, 0, 2, 0, 1)
    next_tables(3)
    for grp in range(GROUPS):
        for j in range(CORES):
            for q in range(seqs):
                ring_copy(0, 1, grp, j, q).wait_send()
    whole(8, sbuf)
    whole(9, sbuf)
    to_head_groups(1, w_key)
    scoped("arrive", arrive, 0, 2, 1, 1)
    next_tables(4)
    for grp in range(GROUPS):
        send_first(1, grp, (1, 0))
    whole(10, pbuf.at[1])
    whole(11, pbuf.at[1])
    scoped("final", arrive, 0, 3, 0, 0)
    to_head_groups(2, w_value)
    prefetch()
    scoped("final", arrive, 0, 3, 1, 0)
    whole(12, pbuf.at[0])
    whole(13, pbuf.at[0])
    scoped("arrive", arrive, 1, 1, 0, 1)
    clear_sums()
    for grp in range(GROUPS):
        for q in range(seqs):
            scoped("take_y", take_y, 0, grp, q)
    scoped("begin", begin_attention, (0, 1), 0)
    attend(1, 3, (0, 1), 0, True)
    scoped("arrive", arrive, 1, 1, 1, 1)
    whole(14, pbuf.at[1])
    whole(15, pbuf.at[1])
    scoped("end", end_attention, 0, (0, 1), 0, True)
    scoped("arrive", arrive, 1, 2, 0, 0)
    scoped("arrive", arrive, 1, 2, 1, 0)
    out_copy(0, (0, 1)).wait()
    clear_sums()
    scoped("final", arrive, 1, 3, 0, 1)
    scoped("take_y", take_y, 1, 0, 0)
    scoped("final", arrive, 1, 3, 1, 1, (0,))
    scoped("take_y", take_y, 1, 0, 1)
    scoped("begin", begin_attention, (0,), head_groups)
    scoped("final", arrive, 1, 3, 1, 1, (1,))
    attend(1, 3, (0,), head_groups, True)
    scoped("end", end_attention, 1, (0,), head_groups, True)
    scoped("take_y", take_y, 1, 1, 0)
    scoped("take_y", take_y, 1, 1, 1)
    scoped("begin", begin_attention, (1,), 2 * head_groups)
    attend(1, 3, (1,), 2 * head_groups, False)
    scoped("end", end_attention, 1, (1,), 2 * head_groups, False)
    for grp in range(GROUPS):
        scoped("out", out_copy(1, (grp,)).wait)

    for m in range(micros):
        for s, b in peers:
            key_copy(m, s, b).wait_send()
    for m, s in units:
        for j in range(CORES):
            table_copy(m, s, j).wait_send()
    for m in range(micros):
        for grp in range(GROUPS):
            for q in range(seqs):
                for s in range(1, chips):
                    for j in range(CORES):
                        if (m, s) != (0, 1):
                            ring_copy(m, s, grp, j, q).wait_send()
                rx_copy(m, grp, q).wait_send()
                if m == micros - 1:
                    y_copy(m, grp, q).wait_send()


def solution(mesh):
    stages = mesh.shape["pp"]
    ep_size = mesh.shape["ep"]
    tok_spec = P("pp", "data", "ep", None, None)
    vec_spec = P("pp", None)
    mat_spec = P("pp", None, None)
    head_spec = P("pp", None, None, None)

    def device_step(expert_out, expert_ids, slot_ids, gate_weights, residual, norm_moe, w_gate, w_up, w_down, norm_attn, w_query, w_key, w_value, w_out):
        micros, experts, slots_total, dim = expert_out.shape[1:]
        heads, head_dim = w_query.shape[2:]
        cap = slots_total // ep_size
        chips = ep_size // CORES
        half = dim // CORES
        seqs, seq_len, top_k = expert_ids.shape[2:]
        tok = seqs * seq_len
        group = tok // GROUPS
        width = 2 * head_dim
        head_groups = heads * head_dim // width

        def by_lane(x):
            return jnp.swapaxes(x[0], -1, -2)

        vmem = pl.BlockSpec(memory_space=pltpu.VMEM)
        anyspace = pl.BlockSpec(memory_space=pl.ANY)
        dma = pltpu.SemaphoreType.DMA
        out, _ = pl.pallas_call(
            functools.partial(boundary_kernel, stages, ep_size, seq_len),
            out_shape=[
                jax.ShapeDtypeStruct((micros, tok, dim), BF16),
                jax.ShapeDtypeStruct((3, head_groups, dim, width), BF16),
            ],
            in_specs=[anyspace, vmem, vmem, vmem, anyspace, vmem, anyspace, anyspace, anyspace, vmem, anyspace, anyspace, anyspace, anyspace],
            out_specs=[anyspace, anyspace],
            scratch_shapes=[
                pltpu.VMEM((chips, CORES, experts, cap, half), BF16),
                pltpu.VMEM((2, CORES, experts, cap, half), BF16),
                pltpu.VMEM((2, 2, PARTS, tok, experts * cap), BF16),
                pltpu.VMEM((GROUPS, CORES, group, half), F32),
                pltpu.VMEM((2, GROUPS, CORES, group, half), F32),
                pltpu.VMEM((micros, chips - 1, GROUPS, CORES, group, half), F32),
                pltpu.VMEM((micros, GROUPS, group, half), F32),
                pltpu.VMEM((GROUPS, group, dim), BF16),
                pltpu.VMEM((micros, tok, dim), BF16),
                pltpu.VMEM((micros * tok, dim), BF16),
                pltpu.VMEM((micros * tok, dim), BF16),
                pltpu.VMEM((3, 3, dim, width), BF16),
                pltpu.VMEM((3, width, dim), BF16),
                pltpu.VMEM((3, 128, heads, head_dim), BF16),
                pltpu.VMEM((3, head_groups, 128, width), BF16),
                pltpu.VMEM((tok, dim), BF16),
                pltpu.VMEM((tok, dim), F32),
                pltpu.VMEM((2, 3, tok, width), BF16),
                pltpu.VMEM((2, tok, width), BF16),
                pltpu.VMEM((micros, GROUPS, 2, top_k, group), F32),
                pltpu.VMEM((micros, GROUPS, chips * CORES, 2, top_k, group), F32),
                pltpu.VMEM((micros, GROUPS, group, chips * CORES * 2 * top_k), F32),
                dma((micros, chips, CORES)), dma((micros, chips, CORES)), dma((2, CORES)),
                dma((micros, chips - 1, GROUPS, CORES, seqs // GROUPS)), dma((micros, chips - 1, GROUPS, CORES, seqs // GROUPS)),
                dma((micros, GROUPS, seqs // GROUPS)), dma((micros, GROUPS, seqs // GROUPS)),
                dma((micros, GROUPS, seqs // GROUPS)), dma((micros, GROUPS, seqs // GROUPS)),
                dma((micros, chips, CORES)), dma((micros, chips, CORES)), dma((3, 4)), dma((3,)), dma((3,)), dma((micros, GROUPS)), dma((1,)),
                pltpu.SemaphoreType.REGULAR((chips,)),
            ],
            compiler_params=pltpu.CompilerParams(collective_id=0, has_side_effects=True, vmem_limit_bytes=67_000_000),
            cost_estimate=pl.CostEstimate(flops=50_000_000_000, bytes_accessed=200_000_000, transcendentals=0),
        )(expert_out[0], by_lane(expert_ids), by_lane(slot_ids), by_lane(gate_weights), residual[0].reshape(micros * tok, dim),
          norm_moe, w_gate[0], w_up[0], w_down[0], norm_attn, w_query[0], w_key[0], w_value[0], w_out[0].reshape(heads * head_dim, dim))
        return out.reshape(1, micros, seqs, seq_len, dim)

    in_specs = (tok_spec,) * 5 + (vec_spec, mat_spec, mat_spec, mat_spec, vec_spec, head_spec, head_spec, head_spec, head_spec)
    return jax.shard_map(device_step, mesh=mesh, in_specs=in_specs, out_specs=tok_spec, check_vma=False)
```
